32 devices in a mesh: shard: 8 (over z, x), tp: 4 (over y, core).
Axes of the slice: x: 2, y: 2, z: 4, core: 2. Of those that a mesh axis runs over, the one named last changes fastest.
Arguments:
- one_gate: float32 [2048, 8192], P('shard', 'tp'), may hold values from -0.1875 to 0.1875
- other_gate: float32 [2048, 8192], P('shard', 'tp'), may hold values from -0.125 to 0.125
- one_up: float32 [2048, 8192], P('shard', 'tp'), may hold values from -0.1875 to 0.1875
- other_up: float32 [2048, 8192], P('shard', 'tp'), may hold values from -0.125 to 0.125
- mix_share: float32 [2048], P('shard'), may hold values from 0.2 to 0.8
- norm_train: float32 [2048], P(('shard', 'tp')), may hold values from 0.25 to 1.75
- norm_step: float32 [2048], P(('shard', 'tp')), may hold values from -0.3 to 0.3
Outputs:
- serve_gate: bfloat16 [2048, 8192], P(None, 'tp')
- serve_up: bfloat16 [2048, 8192], P(None, 'tp')
- factor_gate: float32 [8192], P('tp')
- factor_up: float32 [8192], P('tp')
- serve_norm: bfloat16 [2048], replicated
The draws below stay inside these ranges and needn't reach their ends.
All inputs are finite; a program needn't handle non-finite values.
Results may differ from the reference program's by a relative error of at most 0.0004.
Values may be sent and summed in bfloat16 or wider, within the bound.
A program may use at most 128 MiB of HBM per device.

```python
import jax
import jax.numpy as jnp
from jax import lax

D_MODEL = 2048
D_INNER = 8192


def with_spikes(array, key, source, target, blocks, factor):
    owner, partner = [(jnp.arange(array.shape[axis_at]) // (array.shape[axis_at] // blocks)).reshape([-1 if axis == axis_at else 1 for axis in range(array.ndim)]) for axis_at in (source, target)]
    chosen = jax.random.permutation(key, blocks)[partner]
    strong = (owner == chosen) | (owner == (partner + blocks // 2) % blocks)
    return jnp.where(strong, factor * array, array)


def shard_levels(key, shape, pieces, low, largest):
    level = 1.0
    for axis_at, shards_of in pieces:
        draws = jax.random.uniform(jax.random.fold_in(jax.random.fold_in(key, 6), axis_at), (shards_of,), jnp.float32, low / len(pieces), largest / len(pieces))
        level = level * jnp.repeat(jnp.exp(draws), shape[axis_at] // shards_of).reshape((-1,) + (1,) * (len(shape) - 1 - axis_at))
    return level


def normal_values(stream_key, extent, width, bound, split=(), kind=jnp.bfloat16):
    level = shard_levels(stream_key, extent, split, -0.22, 0.18) if split else 1.0
    values = jax.random.normal(stream_key, extent, jnp.float32) * width * level
    return jnp.minimum(jnp.maximum(values, -bound), bound).astype(kind)


def bell_draw_with(own_key, shape, width, most, split, heavy, held_as=jnp.bfloat16):
    result = width * jax.random.normal(own_key, shape, jnp.float32)
    if split:
        result = result * shard_levels(own_key, shape, split, -0.22, 0.18)
    return jnp.clip(with_spikes(result, jax.random.fold_in(own_key, 3), *heavy), -most, most).astype(held_as)


def setup_inputs(seed: int = 0) -> dict:
    arg_keys = jax.random.split(jax.random.key(seed), 8)
    one_gate = bell_draw_with(arg_keys[0], (D_MODEL, D_INNER), D_MODEL ** -0.5, 0.1875, ((0, 8), (1, 4)), (0, 1, 8, 2.0), jnp.float32)
    other_gate = normal_values(arg_keys[1], (D_MODEL, D_INNER), D_MODEL ** -0.5, 0.125, ((0, 8), (1, 4)), jnp.float32)
    one_up = bell_draw_with(arg_keys[2], (D_MODEL, D_INNER), D_MODEL ** -0.5, 0.1875, ((0, 8), (1, 4)), (0, 1, 8, 2.0), jnp.float32)
    other_up = normal_values(arg_keys[3], (D_MODEL, D_INNER), D_MODEL ** -0.5, 0.125, ((0, 8), (1, 4)), jnp.float32)
    mix_share = jnp.clip(0.2 + 0.6 * jax.random.uniform(arg_keys[4], (D_MODEL,), jnp.float32) ** shard_levels(arg_keys[4], (D_MODEL,), ((0, 8),), -0.2, 0.2), 0.2, 0.8)
    norm_train = jnp.clip(1.0 + 0.15 * jax.random.normal(arg_keys[5], (D_MODEL,), jnp.float32), 0.25, 1.75)
    norm_step = jnp.clip(jax.random.uniform(arg_keys[6], (D_MODEL,), jnp.float32, -0.3, 0.3) * shard_levels(arg_keys[6], (D_MODEL,), ((0, 32),), -0.4, 0.0), -0.3, 0.3)
    return dict(one_gate=one_gate, other_gate=other_gate, one_up=one_up, other_up=other_up, mix_share=mix_share, norm_train=norm_train, norm_step=norm_step)


def reference(one_gate, other_gate, one_up, other_up, mix_share, norm_train, norm_step):
    fresh_gate = mix_share[:, None] * one_gate + (1.0 - mix_share[:, None]) * other_gate
    fresh_up = mix_share[:, None] * one_up + (1.0 - mix_share[:, None]) * other_up
    factor_gate = jnp.sqrt(lax.optimization_barrier(jnp.sum(fresh_gate * fresh_gate, axis=0)))
    serve_gate = (fresh_gate / factor_gate).astype(jnp.bfloat16)
    factor_up = jnp.sqrt(lax.optimization_barrier(jnp.sum(fresh_up * fresh_up, axis=0)))
    serve_up = (fresh_up / factor_up).astype(jnp.bfloat16)
    serve_norm = (norm_train + norm_step).astype(jnp.bfloat16)
    return (serve_gate, serve_up, factor_gate, factor_up, serve_norm)
```

```python
import functools

import jax
import jax.numpy as jnp
import numpy as np
from jax import lax
from jax.experimental import pallas as pl
from jax.experimental.pallas import tpu as pltpu
from jax.sharding import PartitionSpec as P

MESH = pl.DeviceIdType.MESH
UP, DOWN, ACROSS = 0, 1, 2


def crosses(place, m, pieces, j, c):
    last = m - 1
    kept = ((place == 0) & (j == 1)) | ((place == last) & (j == last - 1))
    kept = kept & (c >= pieces // 2)
    return ~(kept | ((place == 1) & (j == 0)) | ((place == last - 1) & (j == last)))


def sent(m, pieces, place):
    last, half = m - 1, pieces // 2
    extra = pieces if last > 1 and place in (0, last) else 0
    inner = pieces - half if last > 1 and place in (1, last - 1) else 0
    up = (place + 1) * pieces * (place != last) + extra * (place == 0) + inner * (place == last - 1)
    down = (m - place) * pieces * (place != 0) + extra * (place == last) + inner * (place == 1)
    across = pieces + sum(
        bool(crosses(np.int64(place), m, pieces, np.int64(j), np.int64(c)))
        for j in range(m) if j != place for c in range(pieces)
    )
    return up, down, across


def gather_kernel(
    n, parts, pieces, one_gate, other_gate, one_up, other_up, mix, train, step,
    held, factor_gate, factor_up, gain,
    ones, others, sums, mix_row, shares, gains, norm, gain_rows,
    in_sem, small_sem, sum_send, sum_recv, norm_sem, send_sem, recv_sem, rest_sem,
):
    me = lax.axis_index("shard")
    part = lax.axis_index("tp")
    m, half = n // 2, pieces // 2
    place, side = me // 2, me % 2
    rows, cols = ones.shape[1:]
    tall = rows // half
    mine = me * parts + part
    lanes = shares.shape[1]

    barrier = pltpu.get_barrier_semaphore()

    @pl.loop(1, n)
    def _(off):
        pl.semaphore_signal(barrier, inc=1, device_id={"shard": lax.rem(me + off, n)}, device_id_type=MESH)

    @pl.loop(1, parts)
    def _(off):
        pl.semaphore_signal(barrier, inc=1, device_id={"tp": lax.rem(part + off, parts)}, device_id_type=MESH)

    read_mix = pltpu.make_async_copy(mix, mix_row, small_sem.at[0])
    read_gains = [
        pltpu.make_async_copy(source, gains.at[i], small_sem.at[1]) for i, source in enumerate((train, step))
    ]

    def reads(piece):
        a, at = piece // half, pl.ds(piece % half * tall, tall)
        first, second = ((one_gate, other_gate), (one_up, other_up))[a]
        return (
            pltpu.make_async_copy(first.at[at], ones.at[a, at], in_sem.at[piece]),
            pltpu.make_async_copy(second.at[at], others.at[a, at], in_sem.at[piece]),
        )

    def took(ref, sem):
        pltpu.make_async_copy(ref, ref, sem).wait()

    read_mix.start()
    for piece in range(half):
        for copy in reads(piece):
            copy.start()
    read_mix.wait()
    shares[...] = jnp.transpose(jnp.broadcast_to(mix_row[...], (lanes, shares.shape[0])))

    def mix_and_sum(a):
        total = jnp.zeros((8, cols), jnp.float32)
        for piece in range(a * half, (a + 1) * half):
            took(ones.at[:, pl.ds(0, tall)], in_sem.at[piece])

            def mixed(r, total):
                at = pl.ds(pl.multiple_of(piece % half * tall + r * 8, 8), 8)
                share = shares[at]
                rest = 1.0 - share
                share, rest = (jnp.concatenate([v] * (cols // lanes), axis=1) for v in (share, rest))
                fresh = share * ones[a, at] + rest * others[a, at]
                ones[a, at] = fresh
                return total + fresh * fresh

            total = lax.fori_loop(0, tall // 8, mixed, total, unroll=4)
        sums[a, me] = jnp.sum(total, axis=0, keepdims=True)

    def sum_copy(a, off):
        return pltpu.make_async_remote_copy(
            src_ref=sums.at[a, me], dst_ref=sums.at[a, me],
            send_sem=sum_send.at[0], recv_sem=sum_recv.at[a],
            device_id={"shard": lax.rem(me + off, n)}, device_id_type=MESH,
        )

    def exchange(a):
        @pl.loop(1, n)
        def _(off):
            sum_copy(a, off).start()

    def scales(a):
        took(sums.at[a, pl.ds(0, n - 1)], sum_recv.at[a])
        factors = jnp.sqrt(lax.fori_loop(1, n, lambda i, t: t + sums[a, i], sums[a, 0]))
        (factor_gate, factor_up)[a][...] = factors
        return jnp.broadcast_to(1.0 / factors, (8, cols))

    def norm_row(off):
        return pltpu.make_async_remote_copy(
            src_ref=norm.at[mine], dst_ref=norm.at[mine],
            send_sem=norm_sem.at[0], recv_sem=norm_sem.at[1],
            device_id={"tp": lax.rem(part + off, parts)}, device_id_type=MESH,
        )

    def norm_group(off):
        return pltpu.make_async_remote_copy(
            src_ref=norm.at[pl.ds(me * parts, parts)], dst_ref=norm.at[pl.ds(me * parts, parts)],
            send_sem=norm_sem.at[0], recv_sem=norm_sem.at[2],
            device_id={"shard": lax.rem(me + off, n)}, device_id_type=MESH,
        )

    def piece_of(j, s, c):
        at = pl.multiple_of((c // half * n + 2 * j + s) * rows + c % half * tall, 8)
        return held.at[pl.ds(at, tall)]

    def send(way, j, s, c, rest=False):
        target = {
            UP: {"shard": lax.rem(me + 2, n)},
            DOWN: {"shard": lax.rem(me + n - 2, n)},
            ACROSS: {"shard": 2 * place + 1 - side},
        }[way]
        block = piece_of(j, s, c)
        return pltpu.make_async_remote_copy(
            src_ref=block, dst_ref=block,
            send_sem=send_sem.at[way], recv_sem=rest_sem.at[0] if rest else recv_sem.at[j, c],
            device_id=target, device_id_type=MESH,
        )

    def arrived(j, s, c):
        took(piece_of(j, s, c), recv_sem.at[j, c])

    last = m - 1
    first_place, last_place = place == 0, place == last

    def own(a):
        scale = scales(a)
        for c in range(a * half, (a + 1) * half):
            at = c % half * tall

            def scaled(r, _):
                here = pl.multiple_of(at + r * 8, 8)
                there = pl.multiple_of((a * n + me) * rows + at + r * 8, 8)
                held[pl.ds(there, 8)] = (ones[a, pl.ds(here, 8)] * scale).astype(jnp.bfloat16)
                return 0

            lax.fori_loop(0, tall // 8, scaled, 0, unroll=4)

            @pl.when(~last_place)
            def _():
                send(UP, place, side, c).start()

            @pl.when(~first_place)
            def _():
                send(DOWN, place, side, c).start()

            send(ACROSS, place, side, c).start()

    mix_and_sum(0)
    pl.semaphore_wait(barrier, n + parts - 2)
    exchange(0)
    for piece in range(half, pieces):
        for copy in reads(piece):
            copy.start()
    for copy in read_gains:
        copy.start()
    own(0)
    took(gains, small_sem.at[1])
    few = gains.shape[2]
    per = lanes // few
    lane = lax.broadcasted_iota(jnp.int32, (1, lanes), 1)
    summed = jnp.concatenate([gains[0] + gains[1]] * per, axis=1)
    norm[mine] = jnp.where(lane // few == mine % per, summed, 0.0)

    @pl.loop(1, parts)
    def _(off):
        norm_row(off).start()

    mix_and_sum(1)
    exchange(1)

    took(norm.at[pl.ds(0, parts - 1)], norm_sem.at[1])

    @pl.loop(1, n)
    def _(off):
        norm_group(off).start()

    own(1)
    took(norm.at[pl.ds(0, (n - 1) * parts)], norm_sem.at[2])

    @pl.loop(0, gain.shape[0])
    def _(r):
        gain_rows[pl.ds(r, 1)] = functools.reduce(lambda t, i: t + norm[r * per + i], range(1, per), norm[r * per])

    gain[...] = gain_rows[...].astype(jnp.bfloat16)

    def ends(b, c):
        return (first_place | last_place) & (b == 1)

    def inner(b, c):
        return ((place == 1) | (place == last - 1)) & (b == last - 1) & (c >= half)

    @pl.loop(0, last * pieces)
    def _(slot):
        b, c = slot // pieces, slot % pieces

        @pl.when(b < place)
        def _():
            j = place - 1 - b
            arrived(j, side, c)

            @pl.when(~last_place)
            def _():
                send(UP, j, side, c).start()

            @pl.when(crosses(place, m, pieces, j, c))
            def _():
                send(ACROSS, j, side, c, True).start()

        @pl.when(b < last - place)
        def _():
            j = place + 1 + b
            arrived(j, side, c)

            @pl.when(~first_place)
            def _():
                send(DOWN, j, side, c).start()

            @pl.when(crosses(place, m, pieces, j, c))
            def _():
                send(ACROSS, j, side, c, True).start()

        @pl.when(ends(b, c) | inner(b, c))
        def _():
            arrived(place, 1 - side, c)

            @pl.when(first_place | (place == last - 1))
            def _():
                send(UP, place, 1 - side, c, True).start()

            @pl.when(last_place | (place == 1))
            def _():
                send(DOWN, place, 1 - side, c, True).start()

    @pl.loop(0, pieces)
    def _(c):
        @pl.when(~(first_place | last_place | (((place == 1) | (place == last - 1)) & (c >= half))))
        def _():
            arrived(place, 1 - side, c)

    took(held.at[pl.ds(0, last * pieces * tall)], rest_sem.at[0])
    took(sums.at[:, pl.ds(0, n - 1)], sum_send.at[0])
    took(norm.at[pl.ds(0, n * parts - 1)], norm_sem.at[0])
    for k in range(m):
        @pl.when(place == k)
        def _(k=k):
            for way, count in enumerate(sent(m, pieces, k)):
                if count:
                    took(held.at[pl.ds(0, count * tall)], send_sem.at[way])


def write_kernel(n, held, factor_gate, factor_up, gain, gate, up, out_gate, out_up, out_gain, sem, small_sem):
    rows = held.shape[0] // (2 * n)
    copies = [
        pltpu.make_async_copy(held.at[pl.ds((a * n + i) * rows, rows)], out.at[pl.ds(i * rows, rows)], sem.at[a, i])
        for i in range(n)
        for a, out in enumerate((gate, up))
    ]
    for i, (source, out) in enumerate(((factor_gate, out_gate), (factor_up, out_up), (gain, out_gain))):
        copies.append(pltpu.make_async_copy(source, out, small_sem.at[i]))
    for copy in copies:
        copy.start()
    for copy in copies:
        copy.wait()


def shards(n, parts, one_gate, other_gate, one_up, other_up, mix_share, norm_train, norm_step):
    rows, cols = one_gate.shape
    few = norm_train.shape[0]
    lanes = 128
    padded = -(-rows // lanes) * lanes
    pieces = 2 * max(1, rows // 64)
    gain_shape = (n * parts * few // lanes, lanes)
    kinds = pltpu.SemaphoreType
    vmem, anywhere = pl.BlockSpec(memory_space=pltpu.VMEM), pl.BlockSpec(memory_space=pl.ANY)
    held, factor_gate, factor_up, gain = pl.pallas_call(
        functools.partial(gather_kernel, n, parts, pieces),
        out_shape=(
            pltpu.VMEM((2 * n * rows, cols), jnp.bfloat16),
            pltpu.VMEM((1, cols), jnp.float32),
            pltpu.VMEM((1, cols), jnp.float32),
            pltpu.VMEM(gain_shape, jnp.bfloat16),
        ),
        in_specs=[pl.BlockSpec(memory_space=pltpu.HBM)] * 7,
        out_specs=(vmem,) * 4,
        scratch_shapes=[
            pltpu.VMEM((2, rows, cols), jnp.float32),
            pltpu.VMEM((2, rows, cols), jnp.float32),
            pltpu.VMEM((2, n, 1, cols), jnp.float32),
            pltpu.VMEM((1, padded), jnp.float32),
            pltpu.VMEM((padded, lanes), jnp.float32),
            pltpu.VMEM((2, 1, few), jnp.float32),
            pltpu.VMEM((n * parts, 1, lanes), jnp.float32),
            pltpu.VMEM(gain_shape, jnp.float32),
            kinds.DMA((pieces,)),
            kinds.DMA((2,)),
            kinds.DMA((1,)),
            kinds.DMA((2,)),
            kinds.DMA((3,)),
            kinds.DMA((3,)),
            kinds.DMA((n // 2, pieces)),
            kinds.DMA((1,)),
        ],
        compiler_params=pltpu.CompilerParams(
            collective_id=0, has_side_effects=True, vmem_limit_bytes=46 * 2**20
        ),
        name="mix_gather",
    )(
        one_gate, other_gate, one_up, other_up,
        jnp.pad(mix_share, (0, padded - rows))[None], norm_train[None], norm_step[None],
    )
    gate, up, factor_gate, factor_up, gain = pl.pallas_call(
        functools.partial(write_kernel, n),
        out_shape=(jax.ShapeDtypeStruct((n * rows, cols), jnp.bfloat16),) * 2
        + (jax.ShapeDtypeStruct((1, cols), jnp.float32),) * 2
        + (jax.ShapeDtypeStruct(gain_shape, jnp.bfloat16),),
        in_specs=[vmem] * 4,
        out_specs=(anywhere,) * 5,
        scratch_shapes=[kinds.DMA((2, n)), kinds.DMA((3,))],
        compiler_params=pltpu.CompilerParams(vmem_limit_bytes=2**20),
        name="write_out",
    )(held, factor_gate, factor_up, gain)
    return gate, up, factor_gate[0], factor_up[0], gain.reshape(-1)


def solution(mesh):
    return jax.shard_map(
        functools.partial(shards, mesh.shape["shard"], mesh.shape["tp"]),
        mesh=mesh,
        in_specs=(
            P("shard", "tp"),
            P("shard", "tp"),
            P("shard", "tp"),
            P("shard", "tp"),
            P("shard"),
            P(("shard", "tp")),
            P(("shard", "tp")),
        ),
        out_specs=(P(None, "tp"), P(None, "tp"), P("tp"), P("tp"), P()),
        check_vma=False,
    )
```

```python
import functools

import jax
import jax.numpy as jnp
import numpy as np
from jax import lax
from jax.experimental import pallas as pl
from jax.experimental.pallas import tpu as pltpu
from jax.sharding import PartitionSpec as P

MESH = pl.DeviceIdType.MESH
UP, DOWN, ACROSS = 0, 1, 2
AHEAD = 3


def crosses(place, m, pieces, j, c):
    last = m - 1
    kept = ((place == 0) & (j == 1)) | ((place == last) & (j == last - 1))
    kept = kept & (c >= pieces // 2)
    return ~(kept | ((place == 1) & (j == 0)) | ((place == last - 1) & (j == last)))


def sent(m, pieces, place):
    last, half = m - 1, pieces // 2
    extra = pieces if last > 1 and place in (0, last) else 0
    inner = pieces - half if last > 1 and place in (1, last - 1) else 0
    up = (place + 1) * pieces * (place != last) + extra * (place == 0) + inner * (place == last - 1)
    down = (m - place) * pieces * (place != 0) + extra * (place == last) + inner * (place == 1)
    across = pieces + sum(
        bool(crosses(np.int64(place), m, pieces, np.int64(j), np.int64(c)))
        for j in range(m) if j != place for c in range(pieces)
    )
    return up, down, across


def gather_kernel(
    n, parts, pieces, ahead, one_gate, other_gate, one_up, other_up, mix, train, step,
    held, factor_gate, factor_up, gain,
    ones, others, sums, mix_row, shares, gains, norm, gain_rows, early,
    early_send, early_recv, in_sem, small_sem, sum_send, sum_recv, norm_sem, send_sem, recv_sem, rest_sem,
):
    me = lax.axis_index("shard")
    part = lax.axis_index("tp")
    m, half = n // 2, pieces // 2
    place, side = me // 2, me % 2
    rows, cols = ones.shape[1:]
    tall = rows // half
    mine = me * parts + part
    lanes = shares.shape[1]

    read_mix = pltpu.make_async_copy(mix, mix_row, small_sem.at[0])
    read_mix.start()
    barrier = pltpu.get_barrier_semaphore()

    @pl.loop(1, n)
    def _(off):
        pl.semaphore_signal(barrier, inc=1, device_id={"shard": lax.rem(me + off, n)}, device_id_type=MESH)

    @pl.loop(1, parts)
    def _(off):
        pl.semaphore_signal(barrier, inc=1, device_id={"tp": lax.rem(part + off, parts)}, device_id_type=MESH)

    read_gains = [
        pltpu.make_async_copy(source, gains.at[i], small_sem.at[1]) for i, source in enumerate((train, step))
    ]

    def reads(piece):
        a, at = piece // half, pl.ds(piece % half * tall, tall)
        first, second = ((one_gate, other_gate), (one_up, other_up))[a]
        return (
            pltpu.make_async_copy(first.at[at], ones.at[a, at], in_sem.at[piece]),
            pltpu.make_async_copy(second.at[at], others.at[a, at], in_sem.at[piece]),
        )

    def took(ref, sem):
        pltpu.make_async_copy(ref, ref, sem).wait()

    for piece in range(half):
        for copy in reads(piece):
            copy.start()
    read_mix.wait()
    shares[...] = jnp.transpose(jnp.broadcast_to(mix_row[...], (lanes, shares.shape[0])))

    def mix_and_sum(a):
        total = jnp.zeros((8, cols), jnp.float32)
        for piece in range(a * half, (a + 1) * half):
            took(ones.at[:, pl.ds(0, tall)], in_sem.at[piece])
            if piece == half - 1:
                for later in range(half, pieces):
                    for copy in reads(later):
                        copy.start()
                for copy in read_gains:
                    copy.start()

            def mixed(r, total):
                at = pl.ds(pl.multiple_of(piece % half * tall + r * 8, 8), 8)
                share = shares[at]
                rest = 1.0 - share
                share, rest = (jnp.concatenate([v] * (cols // lanes), axis=1) for v in (share, rest))
                fresh = share * ones[a, at] + rest * others[a, at]
                ones[a, at] = fresh
                return total + fresh * fresh

            total = lax.fori_loop(0, tall // 8, mixed, total, unroll=4)
        sums[a, me] = jnp.sum(total, axis=0, keepdims=True)

    def sum_copy(a, off):
        return pltpu.make_async_remote_copy(
            src_ref=sums.at[a, me], dst_ref=sums.at[a, me],
            send_sem=sum_send.at[0], recv_sem=sum_recv.at[a],
            device_id={"shard": lax.rem(me + off, n)}, device_id_type=MESH,
        )

    def exchange(a):
        @pl.loop(1, n)
        def _(off):
            sum_copy(a, off).start()

    def scales(a):
        took(sums.at[a, pl.ds(0, n - 1)], sum_recv.at[a])
        factors = jnp.sqrt(lax.fori_loop(1, n, lambda i, t: t + sums[a, i], sums[a, 0]))
        (factor_gate, factor_up)[a][...] = factors
        return jnp.broadcast_to(1.0 / factors, (8, cols))

    def norm_row(off):
        return pltpu.make_async_remote_copy(
            src_ref=norm.at[mine], dst_ref=norm.at[mine],
            send_sem=norm_sem.at[0], recv_sem=norm_sem.at[1],
            device_id={"tp": lax.rem(part + off, parts)}, device_id_type=MESH,
        )

    def norm_group(off):
        return pltpu.make_async_remote_copy(
            src_ref=norm.at[pl.ds(me * parts, parts)], dst_ref=norm.at[pl.ds(me * parts, parts)],
            send_sem=norm_sem.at[0], recv_sem=norm_sem.at[2],
            device_id={"shard": lax.rem(me + off, n)}, device_id_type=MESH,
        )

    def piece_of(j, s, c, skip=0):
        at = pl.multiple_of((c // half * n + 2 * j + s) * rows + c % half * tall + skip, 8)
        return held.at[pl.ds(at, tall - skip)]

    targets = {
        UP: {"shard": lax.rem(me + 2, n)},
        DOWN: {"shard": lax.rem(me + n - 2, n)},
        ACROSS: {"shard": 2 * place + 1 - side},
    }

    def send(way, j, s, c, rest=False, skip=0):
        block = piece_of(j, s, c, skip)
        return pltpu.make_async_remote_copy(
            src_ref=block, dst_ref=block,
            send_sem=send_sem.at[way], recv_sem=rest_sem.at[0] if rest else recv_sem.at[j, c],
            device_id=targets[way], device_id_type=MESH,
        )

    def arrived(j, s, c, first):
        @pl.when(first)
        def _():
            took(piece_of(j, s, c, ahead), recv_sem.at[j, c])

        @pl.when(~first)
        def _():
            took(piece_of(j, s, c), recv_sem.at[j, c])

    def send_early(way):
        return pltpu.make_async_remote_copy(
            src_ref=ones.at[0, pl.ds(0, ahead)], dst_ref=early.at[way],
            send_sem=early_send.at[0], recv_sem=early_recv.at[way],
            device_id=targets[way], device_id_type=MESH,
        )

    def take_early(way, j, s, scale):
        took(early.at[way], early_recv.at[way])
        for r in range(0, ahead, 8):
            there = pl.multiple_of((2 * j + s) * rows + r, 8)
            held[pl.ds(there, 8)] = (early[way, pl.ds(r, 8)] * scale).astype(jnp.bfloat16)

    last = m - 1
    first_place, last_place = place == 0, place == last

    def own(a):
        scale = scales(a)
        for c in range(a * half, (a + 1) * half):
            at = c % half * tall
            skip = ahead if c == 0 else 0

            def scaled(r, _):
                here = pl.multiple_of(at + r * 8, 8)
                there = pl.multiple_of((a * n + me) * rows + at + r * 8, 8)
                held[pl.ds(there, 8)] = (ones[a, pl.ds(here, 8)] * scale).astype(jnp.bfloat16)
                return 0

            lax.fori_loop(skip // 8, tall // 8, scaled, 0, unroll=tall // 8 % 4 == 0 and skip == 0 and 4 or 1)

            @pl.when(~last_place)
            def _():
                send(UP, place, side, c, False, skip).start()

            @pl.when(~first_place)
            def _():
                send(DOWN, place, side, c, False, skip).start()

            send(ACROSS, place, side, c, False, skip).start()
        return scale

    mix_and_sum(0)
    pl.semaphore_wait(barrier, n + parts - 2)
    exchange(0)

    @pl.when(~last_place)
    def _():
        send_early(UP).start()

    @pl.when(~first_place)
    def _():
        send_early(DOWN).start()

    send_early(ACROSS).start()
    mix_and_sum(1)
    exchange(1)
    scale = own(0)
    for r in range(0, ahead, 8):
        there = pl.multiple_of(me * rows + r, 8)
        held[pl.ds(there, 8)] = (ones[0, pl.ds(r, 8)] * scale).astype(jnp.bfloat16)
    took(gains, small_sem.at[1])
    few = gains.shape[2]
    per = lanes // few
    lane = lax.broadcasted_iota(jnp.int32, (1, lanes), 1)
    summed = jnp.concatenate([gains[0] + gains[1]] * per, axis=1)
    norm[mine] = jnp.where(lane // few == mine % per, summed, 0.0)

    @pl.loop(1, parts)
    def _(off):
        norm_row(off).start()

    @pl.when(~first_place)
    def _():
        take_early(UP, place - 1, side, scale)

    @pl.when(~last_place)
    def _():
        take_early(DOWN, place + 1, side, scale)

    take_early(ACROSS, place, 1 - side, scale)
    own(1)
    took(norm.at[pl.ds(0, parts - 1)], norm_sem.at[1])

    @pl.loop(1, n)
    def _(off):
        norm_group(off).start()

    def ends(b, c):
        return (first_place | last_place) & (b == 1)

    def inner(b, c):
        return ((place == 1) | (place == last - 1)) & (b == last - 1) & (c >= half)

    @pl.loop(0, last * pieces)
    def _(slot):
        b, c = slot // pieces, slot % pieces

        @pl.when(b < place)
        def _():
            j = place - 1 - b
            arrived(j, side, c, (b == 0) & (c == 0))

            @pl.when(~last_place)
            def _():
                send(UP, j, side, c).start()

            @pl.when(crosses(place, m, pieces, j, c))
            def _():
                send(ACROSS, j, side, c, True).start()

        @pl.when(b < last - place)
        def _():
            j = place + 1 + b
            arrived(j, side, c, (b == 0) & (c == 0))

            @pl.when(~first_place)
            def _():
                send(DOWN, j, side, c).start()

            @pl.when(crosses(place, m, pieces, j, c))
            def _():
                send(ACROSS, j, side, c, True).start()

        @pl.when(ends(b, c) | inner(b, c))
        def _():
            arrived(place, 1 - side, c, c == 0)

            @pl.when(first_place | (place == last - 1))
            def _():
                send(UP, place, 1 - side, c, True).start()

            @pl.when(last_place | (place == 1))
            def _():
                send(DOWN, place, 1 - side, c, True).start()

    took(norm.at[pl.ds(0, (n - 1) * parts)], norm_sem.at[2])

    @pl.loop(0, gain.shape[0])
    def _(r):
        gain_rows[pl.ds(r, 1)] = functools.reduce(lambda t, i: t + norm[r * per + i], range(1, per), norm[r * per])

    gain[...] = gain_rows[...].astype(jnp.bfloat16)

    @pl.loop(0, pieces)
    def _(c):
        @pl.when(~(first_place | last_place | (((place == 1) | (place == last - 1)) & (c >= half))))
        def _():
            arrived(place, 1 - side, c, c == 0)

    took(held.at[pl.ds(0, last * pieces * tall)], rest_sem.at[0])
    took(sums.at[:, pl.ds(0, n - 1)], sum_send.at[0])
    took(norm.at[pl.ds(0, n * parts - 1)], norm_sem.at[0])

    @pl.when(first_place | last_place)
    def _():
        took(early.at[pl.ds(0, 2)], early_send.at[0])

    @pl.when(~(first_place | last_place))
    def _():
        took(early, early_send.at[0])

    for k in range(m):
        @pl.when(place == k)
        def _(k=k):
            for way, count in enumerate(sent(m, pieces, k)):
                if count:
                    took(held.at[pl.ds(0, count * tall - ahead)], send_sem.at[way])


def write_kernel(n, held, factor_gate, factor_up, gain, gate, up, out_gate, out_up, out_gain, sem, small_sem):
    rows = held.shape[0] // (2 * n)
    copies = [
        pltpu.make_async_copy(held.at[pl.ds((a * n + i) * rows, rows)], out.at[pl.ds(i * rows, rows)], sem.at[a, i])
        for i in range(n)
        for a, out in enumerate((gate, up))
    ]
    for i, (source, out) in enumerate(((factor_gate, out_gate), (factor_up, out_up), (gain, out_gain))):
        copies.append(pltpu.make_async_copy(source, out, small_sem.at[i]))
    for copy in copies:
        copy.start()
    for copy in copies:
        copy.wait()


def shards(n, parts, one_gate, other_gate, one_up, other_up, mix_share, norm_train, norm_step):
    rows, cols = one_gate.shape
    few = norm_train.shape[0]
    lanes = 128
    padded = -(-rows // lanes) * lanes
    pieces = 2 * max(1, rows // 64)
    ahead = rows // (pieces // 2) // 8 * AHEAD // 8 * 8
    gain_shape = (n * parts * few // lanes, lanes)
    kinds = pltpu.SemaphoreType
    vmem, anywhere = pl.BlockSpec(memory_space=pltpu.VMEM), pl.BlockSpec(memory_space=pl.ANY)
    held, factor_gate, factor_up, gain = pl.pallas_call(
        functools.partial(gather_kernel, n, parts, pieces, ahead),
        out_shape=(
            pltpu.VMEM((2 * n * rows, cols), jnp.bfloat16),
            pltpu.VMEM((1, cols), jnp.float32),
            pltpu.VMEM((1, cols), jnp.float32),
            pltpu.VMEM(gain_shape, jnp.bfloat16),
        ),
        in_specs=[pl.BlockSpec(memory_space=pltpu.HBM)] * 7,
        out_specs=(vmem,) * 4,
        scratch_shapes=[
            pltpu.VMEM((2, rows, cols), jnp.float32),
            pltpu.VMEM((2, rows, cols), jnp.float32),
            pltpu.VMEM((2, n, 1, cols), jnp.float32),
            pltpu.VMEM((1, padded), jnp.float32),
            pltpu.VMEM((padded, lanes), jnp.float32),
            pltpu.VMEM((2, 1, few), jnp.float32),
            pltpu.VMEM((n * parts, 1, lanes), jnp.float32),
            pltpu.VMEM(gain_shape, jnp.float32),
            pltpu.VMEM((3, ahead, cols), jnp.float32),
            kinds.DMA((1,)),
            kinds.DMA((3,)),
            kinds.DMA((pieces,)),
            kinds.DMA((2,)),
            kinds.DMA((1,)),
            kinds.DMA((2,)),
            kinds.DMA((3,)),
            kinds.DMA((3,)),
            kinds.DMA((n // 2, pieces)),
            kinds.DMA((1,)),
        ],
        compiler_params=pltpu.CompilerParams(
            collective_id=0, has_side_effects=True, vmem_limit_bytes=46 * 2**20
        ),
        name="mix_gather",
    )(
        one_gate, other_gate, one_up, other_up,
        jnp.pad(mix_share, (0, padded - rows))[None], norm_train[None], norm_step[None],
    )
    gate, up, factor_gate, factor_up, gain = pl.pallas_call(
        functools.partial(write_kernel, n),
        out_shape=(jax.ShapeDtypeStruct((n * rows, cols), jnp.bfloat16),) * 2
        + (jax.ShapeDtypeStruct((1, cols), jnp.float32),) * 2
        + (jax.ShapeDtypeStruct(gain_shape, jnp.bfloat16),),
        in_specs=[vmem] * 4,
        out_specs=(anywhere,) * 5,
        scratch_shapes=[kinds.DMA((2, n)), kinds.DMA((3,))],
        compiler_params=pltpu.CompilerParams(vmem_limit_bytes=2**20),
        name="write_out",
    )(held, factor_gate, factor_up, gain)
    return gate, up, factor_gate[0], factor_up[0], gain.reshape(-1)


def solution(mesh):
    return jax.shard_map(
        functools.partial(shards, mesh.shape["shard"], mesh.shape["tp"]),
        mesh=mesh,
        in_specs=(
            P("shard", "tp"),
            P("shard", "tp"),
            P("shard", "tp"),
            P("shard", "tp"),
            P("shard"),
            P(("shard", "tp")),
            P(("shard", "tp")),
        ),
        out_specs=(P(None, "tp"), P(None, "tp"), P("tp"), P("tp"), P()),
        check_vma=False,
    )
```

```python
import functools

import jax
import jax.numpy as jnp
import numpy as np
from jax import lax
from jax.experimental import pallas as pl
from jax.experimental.pallas import tpu as pltpu
from jax.sharding import PartitionSpec as P

MESH = pl.DeviceIdType.MESH
UP, DOWN, ACROSS = 0, 1, 2
AHEAD = 2


def crosses(place, m, pieces, j, c):
    last = m - 1
    kept = ((place == 0) & (j == 1)) | ((place == last) & (j == last - 1))
    kept = kept & (c >= pieces // 2)
    return ~(kept | ((place == 1) & (j == 0)) | ((place == last - 1) & (j == last)))


def sent(m, pieces, place):
    last, half = m - 1, pieces // 2
    extra = pieces if last > 1 and place in (0, last) else 0
    inner = pieces - half if last > 1 and place in (1, last - 1) else 0
    up = (place + 1) * pieces * (place != last) + extra * (place == 0) + inner * (place == last - 1)
    down = (m - place) * pieces * (place != 0) + extra * (place == last) + inner * (place == 1)
    across = pieces + sum(
        bool(crosses(np.int64(place), m, pieces, np.int64(j), np.int64(c)))
        for j in range(m) if j != place for c in range(pieces)
    )
    return up, down, across


def gather_kernel(
    n, parts, pieces, ahead, one_gate, other_gate, one_up, other_up, mix, train, step,
    held, factor_gate, factor_up, gain,
    ones, others, sums, mix_row, shares, gains, norm, gain_rows, early,
    early_send, early_recv, in_sem, small_sem, sum_send, sum_recv, norm_sem, send_sem, recv_sem, rest_sem,
):
    me = lax.axis_index("shard")
    part = lax.axis_index("tp")
    m, half = n // 2, pieces // 2
    place, side = me // 2, me % 2
    rows, cols = ones.shape[1:]
    tall = rows // half
    mine = me * parts + part
    lanes = shares.shape[1]

    read_mix = pltpu.make_async_copy(mix, mix_row, small_sem.at[0])
    read_mix.start()
    barrier = pltpu.get_barrier_semaphore()

    @pl.loop(1, n)
    def _(off):
        pl.semaphore_signal(barrier, inc=1, device_id={"shard": lax.rem(me + off, n)}, device_id_type=MESH)

    @pl.loop(1, parts)
    def _(off):
        pl.semaphore_signal(barrier, inc=1, device_id={"tp": lax.rem(part + off, parts)}, device_id_type=MESH)

    read_gains = [
        pltpu.make_async_copy(source, gains.at[i], small_sem.at[1]) for i, source in enumerate((train, step))
    ]

    def reads(piece):
        a, at = piece // half, pl.ds(piece % half * tall, tall)
        first, second = ((one_gate, other_gate), (one_up, other_up))[a]
        return (
            pltpu.make_async_copy(first.at[at], ones.at[a, at], in_sem.at[piece]),
            pltpu.make_async_copy(second.at[at], others.at[a, at], in_sem.at[piece]),
        )

    def took(ref, sem):
        pltpu.make_async_copy(ref, ref, sem).wait()

    for piece in range(half):
        for copy in reads(piece):
            copy.start()
    read_mix.wait()
    shares[...] = jnp.transpose(jnp.broadcast_to(mix_row[...], (lanes, shares.shape[0])))

    def mix_and_sum(a):
        total = jnp.zeros((8, cols), jnp.float32)
        for piece in range(a * half, (a + 1) * half):
            took(ones.at[:, pl.ds(0, tall)], in_sem.at[piece])
            if piece == half - 1:
                for later in range(half, pieces):
                    for copy in reads(later):
                        copy.start()
                for copy in read_gains:
                    copy.start()

            def mixed(r, total):
                at = pl.ds(pl.multiple_of(piece % half * tall + r * 8, 8), 8)
                share = shares[at]
                rest = 1.0 - share
                share, rest = (jnp.concatenate([v] * (cols // lanes), axis=1) for v in (share, rest))
                fresh = share * ones[a, at] + rest * others[a, at]
                ones[a, at] = fresh
                return total + fresh * fresh

            total = lax.fori_loop(0, tall // 8, mixed, total, unroll=4)
        sums[(me, n + m)[a]] = jnp.sum(total, axis=0, keepdims=True)

    def sum_copy(source, target, recv, **device_id):
        return pltpu.make_async_remote_copy(
            src_ref=sums.at[source], dst_ref=sums.at[target],
            send_sem=sum_send.at[0], recv_sem=sum_recv.at[recv],
            device_id=device_id, device_id_type=MESH,
        )

    def exchange_up():
        took(sums.at[0], sum_recv.at[2])
        sums[n + place] = sums[n + m] + sums[n + m + 1]

        @pl.loop(1, m)
        def _(off):
            sum_copy(n + place, n + place, 1, shard=lax.rem(me + 2 * off, n)).start()

    def scales(a):
        first, count = ((0, n), (n, m))[a]
        took(sums.at[pl.ds(0, count - 1)], sum_recv.at[a])
        factors = jnp.sqrt(lax.fori_loop(1, count, lambda i, t: t + sums[first + i], sums[first]))
        (factor_gate, factor_up)[a][...] = factors
        return jnp.broadcast_to(1.0 / factors, (8, cols))

    def norm_row(off):
        return pltpu.make_async_remote_copy(
            src_ref=norm.at[mine], dst_ref=norm.at[mine],
            send_sem=norm_sem.at[0], recv_sem=norm_sem.at[1],
            device_id={"tp": lax.rem(part + off, parts)}, device_id_type=MESH,
        )

    def norm_group(off):
        return pltpu.make_async_remote_copy(
            src_ref=norm.at[pl.ds(me * parts, parts)], dst_ref=norm.at[pl.ds(me * parts, parts)],
            send_sem=norm_sem.at[0], recv_sem=norm_sem.at[2],
            device_id={"shard": lax.rem(me + off, n)}, device_id_type=MESH,
        )

    def piece_of(j, s, c, skip=0):
        at = pl.multiple_of((c // half * n + 2 * j + s) * rows + c % half * tall + skip, 8)
        return held.at[pl.ds(at, tall - skip)]

    targets = {
        UP: {"shard": lax.rem(me + 2, n)},
        DOWN: {"shard": lax.rem(me + n - 2, n)},
        ACROSS: {"shard": 2 * place + 1 - side},
    }

    def send(way, j, s, c, rest=False, skip=0):
        block = piece_of(j, s, c, skip)
        return pltpu.make_async_remote_copy(
            src_ref=block, dst_ref=block,
            send_sem=send_sem.at[way], recv_sem=rest_sem.at[0] if rest else recv_sem.at[j, c],
            device_id=targets[way], device_id_type=MESH,
        )

    def arrived(j, s, c, first):
        @pl.when(first)
        def _():
            took(piece_of(j, s, c, ahead), recv_sem.at[j, c])

        @pl.when(~first)
        def _():
            took(piece_of(j, s, c), recv_sem.at[j, c])

    def send_early(way):
        return pltpu.make_async_remote_copy(
            src_ref=ones.at[0, pl.ds(0, ahead)], dst_ref=early.at[way],
            send_sem=early_send.at[0], recv_sem=early_recv.at[way],
            device_id=targets[way], device_id_type=MESH,
        )

    def take_early(way, j, s, scale):
        took(early.at[way], early_recv.at[way])
        for r in range(0, ahead, 8):
            there = pl.multiple_of((2 * j + s) * rows + r, 8)
            held[pl.ds(there, 8)] = (early[way, pl.ds(r, 8)] * scale).astype(jnp.bfloat16)

    last = m - 1
    first_place, last_place = place == 0, place == last

    def own(a):
        scale = scales(a)
        for c in range(a * half, (a + 1) * half):
            at = c % half * tall
            skip = ahead if c == 0 else 0

            def scaled(r, _):
                here = pl.multiple_of(at + r * 8, 8)
                there = pl.multiple_of((a * n + me) * rows + at + r * 8, 8)
                held[pl.ds(there, 8)] = (ones[a, pl.ds(here, 8)] * scale).astype(jnp.bfloat16)
                return 0

            lax.fori_loop(skip // 8, tall // 8, scaled, 0, unroll=tall // 8 % 4 == 0 and skip == 0 and 4 or 1)

            @pl.when(~last_place)
            def _():
                send(UP, place, side, c, False, skip).start()

            @pl.when(~first_place)
            def _():
                send(DOWN, place, side, c, False, skip).start()

            send(ACROSS, place, side, c, False, skip).start()
            if c == (half - 1) // 2:
                exchange_up()
        return scale

    mix_and_sum(0)
    pl.semaphore_wait(barrier, n + parts - 2)

    @pl.loop(1, n)
    def _(off):
        sum_copy(me, me, 0, shard=lax.rem(me + off, n)).start()

    @pl.when(~last_place)
    def _():
        send_early(UP).start()

    @pl.when(~first_place)
    def _():
        send_early(DOWN).start()

    send_early(ACROSS).start()
    mix_and_sum(1)
    sum_copy(n + m, n + m + 1, 2, **targets[ACROSS]).start()
    scale = own(0)
    for r in range(0, ahead, 8):
        there = pl.multiple_of(me * rows + r, 8)
        held[pl.ds(there, 8)] = (ones[0, pl.ds(r, 8)] * scale).astype(jnp.bfloat16)
    took(gains, small_sem.at[1])
    few = gains.shape[2]
    per = lanes // few
    lane = lax.broadcasted_iota(jnp.int32, (1, lanes), 1)
    summed = jnp.concatenate([gains[0] + gains[1]] * per, axis=1)
    norm[mine] = jnp.where(lane // few == mine % per, summed, 0.0)

    @pl.loop(1, parts)
    def _(off):
        norm_row(off).start()

    @pl.when(~first_place)
    def _():
        take_early(UP, place - 1, side, scale)

    @pl.when(~last_place)
    def _():
        take_early(DOWN, place + 1, side, scale)

    take_early(ACROSS, place, 1 - side, scale)
    own(1)
    took(norm.at[pl.ds(0, parts - 1)], norm_sem.at[1])

    @pl.loop(1, n)
    def _(off):
        norm_group(off).start()

    def ends(b, c):
        return (first_place | last_place) & (b == 1)

    def inner(b, c):
        return ((place == 1) | (place == last - 1)) & (b == last - 1) & (c >= half)

    @pl.loop(0, last * pieces)
    def _(slot):
        b, c = slot // pieces, slot % pieces

        @pl.when(b < place)
        def _():
            j = place - 1 - b
            arrived(j, side, c, (b == 0) & (c == 0))

            @pl.when(~last_place)
            def _():
                send(UP, j, side, c).start()

            @pl.when(crosses(place, m, pieces, j, c))
            def _():
                send(ACROSS, j, side, c, True).start()

        @pl.when(b < last - place)
        def _():
            j = place + 1 + b
            arrived(j, side, c, (b == 0) & (c == 0))

            @pl.when(~first_place)
            def _():
                send(DOWN, j, side, c).start()

            @pl.when(crosses(place, m, pieces, j, c))
            def _():
                send(ACROSS, j, side, c, True).start()

        @pl.when(ends(b, c) | inner(b, c))
        def _():
            arrived(place, 1 - side, c, c == 0)

            @pl.when(first_place | (place == last - 1))
            def _():
                send(UP, place, 1 - side, c, True).start()

            @pl.when(last_place | (place == 1))
            def _():
                send(DOWN, place, 1 - side, c, True).start()

    took(norm.at[pl.ds(0, (n - 1) * parts)], norm_sem.at[2])

    @pl.loop(0, gain.shape[0])
    def _(r):
        gain_rows[pl.ds(r, 1)] = functools.reduce(lambda t, i: t + norm[r * per + i], range(1, per), norm[r * per])

    gain[...] = gain_rows[...].astype(jnp.bfloat16)

    @pl.loop(0, pieces)
    def _(c):
        @pl.when(~(first_place | last_place | (((place == 1) | (place == last - 1)) & (c >= half))))
        def _():
            arrived(place, 1 - side, c, c == 0)

    took(held.at[pl.ds(0, last * pieces * tall)], rest_sem.at[0])
    took(sums.at[pl.ds(0, n - 1 + m)], sum_send.at[0])
    took(norm.at[pl.ds(0, n * parts - 1)], norm_sem.at[0])

    @pl.when(first_place | last_place)
    def _():
        took(early.at[pl.ds(0, 2)], early_send.at[0])

    @pl.when(~(first_place | last_place))
    def _():
        took(early, early_send.at[0])

    for k in range(m):
        @pl.when(place == k)
        def _(k=k):
            for way, count in enumerate(sent(m, pieces, k)):
                if count:
                    took(held.at[pl.ds(0, count * tall - ahead)], send_sem.at[way])


def write_kernel(held, factor_gate, factor_up, gain, gate, up, out_gate, out_up, out_gain, sem, small_sem):
    half = gate.shape[0]
    tall = 64

    @pl.loop(0, half // tall)
    def _(i):
        at = pl.multiple_of(i * tall, tall)
        for a, out in enumerate((gate, up)):
            pltpu.make_async_copy(held.at[pl.ds(a * half + at, tall)], out.at[pl.ds(at, tall)], sem.at[0]).start()

    copies = [
        pltpu.make_async_copy(source, out, small_sem.at[i])
        for i, (source, out) in enumerate(((factor_gate, out_gate), (factor_up, out_up), (gain, out_gain)))
    ]
    for copy in copies:
        copy.start()
    for copy in copies:
        copy.wait()
    pltpu.make_async_copy(held, held, sem.at[0]).wait()


def shards(n, parts, one_gate, other_gate, one_up, other_up, mix_share, norm_train, norm_step):
    rows, cols = one_gate.shape
    few = norm_train.shape[0]
    lanes = 128
    padded = -(-rows // lanes) * lanes
    pieces = 2 * max(1, rows // 64)
    ahead = rows // (pieces // 2) // 8 * AHEAD // 8 * 8
    gain_shape = (n * parts * few // lanes, lanes)
    kinds = pltpu.SemaphoreType
    vmem, anywhere = pl.BlockSpec(memory_space=pltpu.VMEM), pl.BlockSpec(memory_space=pl.ANY)
    held, factor_gate, factor_up, gain = pl.pallas_call(
        functools.partial(gather_kernel, n, parts, pieces, ahead),
        out_shape=(
            pltpu.VMEM((2 * n * rows, cols), jnp.bfloat16),
            pltpu.VMEM((1, cols), jnp.float32),
            pltpu.VMEM((1, cols), jnp.float32),
            pltpu.VMEM(gain_shape, jnp.bfloat16),
        ),
        in_specs=[pl.BlockSpec(memory_space=pltpu.HBM)] * 7,
        out_specs=(vmem,) * 4,
        scratch_shapes=[
            pltpu.VMEM((2, rows, cols), jnp.float32),
            pltpu.VMEM((2, rows, cols), jnp.float32),
            pltpu.VMEM((n + n // 2 + 2, 1, cols), jnp.float32),
            pltpu.VMEM((1, padded), jnp.float32),
            pltpu.VMEM((padded, lanes), jnp.float32),
            pltpu.VMEM((2, 1, few), jnp.float32),
            pltpu.VMEM((n * parts, 1, lanes), jnp.float32),
            pltpu.VMEM(gain_shape, jnp.float32),
            pltpu.VMEM((3, ahead, cols), jnp.float32),
            kinds.DMA((1,)),
            kinds.DMA((3,)),
            kinds.DMA((pieces,)),
            kinds.DMA((2,)),
            kinds.DMA((1,)),
            kinds.DMA((3,)),
            kinds.DMA((3,)),
            kinds.DMA((3,)),
            kinds.DMA((n // 2, pieces)),
            kinds.DMA((1,)),
        ],
        compiler_params=pltpu.CompilerParams(
            collective_id=0, has_side_effects=True, vmem_limit_bytes=46 * 2**20
        ),
        name="mix_gather",
    )(
        one_gate, other_gate, one_up, other_up,
        jnp.pad(mix_share, (0, padded - rows))[None], norm_train[None], norm_step[None],
    )
    gate, up, factor_gate, factor_up, gain = pl.pallas_call(
        write_kernel,
        out_shape=(jax.ShapeDtypeStruct((n * rows, cols), jnp.bfloat16),) * 2
        + (jax.ShapeDtypeStruct((1, cols), jnp.float32),) * 2
        + (jax.ShapeDtypeStruct(gain_shape, jnp.bfloat16),),
        in_specs=[vmem] * 4,
        out_specs=(anywhere,) * 5,
        scratch_shapes=[kinds.DMA((1,)), kinds.DMA((3,))],
        compiler_params=pltpu.CompilerParams(vmem_limit_bytes=2**20),
        name="write_out",
    )(held, factor_gate, factor_up, gain)
    return gate, up, factor_gate[0], factor_up[0], gain.reshape(-1)


def solution(mesh):
    return jax.shard_map(
        functools.partial(shards, mesh.shape["shard"], mesh.shape["tp"]),
        mesh=mesh,
        in_specs=(
            P("shard", "tp"),
            P("shard", "tp"),
            P("shard", "tp"),
            P("shard", "tp"),
            P("shard"),
            P(("shard", "tp")),
            P(("shard", "tp")),
        ),
        out_specs=(P(None, "tp"), P(None, "tp"), P("tp"), P("tp"), P()),
        check_vma=False,
    )
```

```python
import functools

import jax
import jax.numpy as jnp
import numpy as np
from jax import lax
from jax.experimental import pallas as pl
from jax.experimental.pallas import tpu as pltpu
from jax.sharding import PartitionSpec as P

MESH = pl.DeviceIdType.MESH
UP, DOWN, ACROSS = 0, 1, 2
CUTS = (12, 14)


def crosses(place, m, j, c):
    last = m - 1
    kept = ((place == 0) & (j == 1)) | ((place == last) & (j == last - 1))
    kept = kept & (c % 2 == 1)
    return ~(kept | ((place == 1) & (j == 0)) | ((place == last - 1) & (j == last)))


def sent(m, lo, hi, place):
    last, count = m - 1, hi - lo
    extra = count if place in (0, last) else 0
    inner = sum(c % 2 for c in range(lo, hi)) if place in (1, last - 1) else 0
    up = (place + 1) * count * (place != last) + extra * (place == 0) + inner * (place == last - 1)
    down = (m - place) * count * (place != 0) + extra * (place == last) + inner * (place == 1)
    across = count + sum(
        bool(crosses(np.int64(place), m, np.int64(j), np.int64(c)))
        for j in range(m) if j != place for c in range(lo, hi)
    )
    return up, down, across


def cuts_of(pieces):
    return tuple(min(max(1, pieces * cut // 16), pieces - 1) for cut in CUTS)


def took(ref, sem):
    pltpu.make_async_copy(ref, ref, sem).wait()


class Line:
    def __init__(self, n, pieces, rows, ranges, own, land, send_sem, recv_sem, rest_sem, ahead):
        self.n, self.m, self.half = n, n // 2, pieces // 2
        self.rows, self.tall, self.ranges, self.ahead = rows, rows // (pieces // 2), ranges, ahead
        self.me = lax.axis_index("shard")
        self.place, self.side = self.me // 2, self.me % 2
        self.turn = lax.axis_index("tp") % 2
        self.lo, self.hi = (jnp.where(self.turn == 0, first, second) for first, second in zip(*ranges))
        self.base = min(lo for lo, _ in ranges)
        self.own, self.land = own, land
        self.send_sem, self.recv_sem, self.rest_sem = send_sem, recv_sem, rest_sem
        self.first, self.last = self.place == 0, self.place == self.m - 1
        me = self.me
        self.targets = {
            UP: {"shard": lax.rem(me + 2, n)},
            DOWN: {"shard": lax.rem(me + n - 2, n)},
            ACROSS: {"shard": 2 * self.place + 1 - self.side},
        }

    def greet(self, others):
        barrier = pltpu.get_barrier_semaphore()
        for way, unless in ((UP, self.last), (DOWN, self.first), (ACROSS, self.place < 0)):
            @pl.when(~unless)
            def _(way=way):
                pl.semaphore_signal(barrier, inc=1, device_id=self.targets[way], device_id_type=MESH)

        ends = self.first | self.last

        def wait():
            @pl.when(ends)
            def _():
                pl.semaphore_wait(barrier, 2 + others)

            @pl.when(~ends)
            def _():
                pl.semaphore_wait(barrier, 3 + others)

        return wait

    def piece(self, ref, j, s, c, skip=0):
        at = (c // self.half * self.n + 2 * j + s) * self.rows + c % self.half * self.tall + skip
        return ref.at[pl.ds(pl.multiple_of(at, 8), self.tall - skip)]

    def send(self, way, j, s, c, rest=False, skip=0, own=False):
        own = own and self.own is not None
        source = self.own.at[pl.ds(pl.multiple_of((c - self.base) * self.tall, 8), self.tall)] if own else None
        return pltpu.make_async_remote_copy(
            src_ref=self.piece(self.land, j, s, c, skip) if source is None else source,
            dst_ref=self.piece(self.land, j, s, c, skip),
            send_sem=self.send_sem.at[way],
            recv_sem=self.rest_sem.at[0] if rest else self.recv_sem.at[j, c - self.base],
            device_id=self.targets[way], device_id_type=MESH,
        )

    def send_own(self, c, skip=0):
        @pl.when(~self.last)
        def _():
            self.send(UP, self.place, self.side, c, False, skip, True).start()

        @pl.when(~self.first)
        def _():
            self.send(DOWN, self.place, self.side, c, False, skip, True).start()

        self.send(ACROSS, self.place, self.side, c, False, skip, True).start()

    def arrived(self, j, s, c, first):
        def whole():
            took(self.piece(self.land, j, s, c), self.recv_sem.at[j, c - self.base])

        if not self.ahead:
            return whole()

        @pl.when(first)
        def _():
            took(self.piece(self.land, j, s, c, self.ahead), self.recv_sem.at[j, c - self.base])

        pl.when(~first)(whole)

    def relay(self):
        place, side, m, last = self.place, self.side, self.m, self.m - 1
        ends, inner = self.first | self.last, (place == 1) | (place == last - 1)

        @pl.loop(0, last)
        def _(b):
            @pl.loop(self.lo, self.hi)
            def _(c):
                def pass_on(way, j, stop):
                    self.arrived(j, side, c, (b == 0) & (c == 0))

                    @pl.when(~stop)
                    def _():
                        self.send(way, j, side, c).start()

                    @pl.when(crosses(place, m, j, c))
                    def _():
                        self.send(ACROSS, j, side, c, True).start()

                @pl.when(b < place)
                def _():
                    pass_on(UP, place - 1 - b, self.last)

                @pl.when(b < last - place)
                def _():
                    pass_on(DOWN, place + 1 + b, self.first)

                @pl.when((ends & (b == 1)) | (inner & (b == last - 1) & (c % 2 == 1)))
                def _():
                    self.arrived(place, 1 - side, c, c == 0)

                    @pl.when(self.first | (place == last - 1))
                    def _():
                        self.send(UP, place, 1 - side, c, True).start()

                    @pl.when(self.last | (place == 1))
                    def _():
                        self.send(DOWN, place, 1 - side, c, True).start()

    def finish(self):
        place, side, last = self.place, self.side, self.m - 1
        ends, inner = self.first | self.last, (place == 1) | (place == last - 1)

        @pl.loop(self.lo, self.hi)
        def _(c):
            @pl.when(~(ends | (inner & (c % 2 == 1))))
            def _():
                self.arrived(place, 1 - side, c, c == 0)

        for turn, (lo, hi) in enumerate(self.ranges):
            @pl.when(self.turn == turn)
            def _(lo=lo, hi=hi):
                took(self.land.at[pl.ds(0, last * (hi - lo) * self.tall)], self.rest_sem.at[0])
                for k in range(self.m):
                    @pl.when(place == k)
                    def _(k=k):
                        for way, count in enumerate(sent(self.m, lo, hi, k)):
                            if count:
                                took(self.land.at[pl.ds(0, count * self.tall - self.ahead)], self.send_sem.at[way])


def gather_kernel(
    n, parts, pieces, ahead, cuts, one_gate, other_gate, one_up, other_up, mix, train, step,
    held, left, factor_gate, factor_up, gain,
    ones, others, sums, mix_row, shares, gains, norm, gain_rows, early,
    early_send, early_recv, in_sem, small_sem, sum_send, sum_recv, norm_sem, send_sem, recv_sem, rest_sem,
):
    me = lax.axis_index("shard")
    part = lax.axis_index("tp")
    m, half = n // 2, pieces // 2
    place, side = me // 2, me % 2
    rows, cols = ones.shape[1:]
    tall = rows // half
    mine = me * parts + part
    ranges = tuple((0, cut) for cut in cuts)
    line = Line(n, pieces, rows, ranges, None, held, send_sem, recv_sem, rest_sem, ahead)
    targets, first_place, last_place = line.targets, line.first, line.last
    lanes = shares.shape[1]

    read_mix = pltpu.make_async_copy(mix, mix_row, small_sem.at[0])
    read_mix.start()
    barrier = pltpu.get_barrier_semaphore()

    @pl.loop(1, n)
    def _(off):
        pl.semaphore_signal(barrier, inc=1, device_id={"shard": lax.rem(me + off, n)}, device_id_type=MESH)

    @pl.loop(1, parts)
    def _(off):
        pl.semaphore_signal(barrier, inc=1, device_id={"tp": lax.rem(part + off, parts)}, device_id_type=MESH)

    read_gains = [
        pltpu.make_async_copy(source, gains.at[i], small_sem.at[1]) for i, source in enumerate((train, step))
    ]

    def reads(piece):
        a, at = piece // half, pl.ds(piece % half * tall, tall)
        first, second = ((one_gate, other_gate), (one_up, other_up))[a]
        return (
            pltpu.make_async_copy(first.at[at], ones.at[a, at], in_sem.at[piece]),
            pltpu.make_async_copy(second.at[at], others.at[a, at], in_sem.at[piece]),
        )

    for piece in range(half):
        for copy in reads(piece):
            copy.start()
    read_mix.wait()
    shares[...] = jnp.transpose(jnp.broadcast_to(mix_row[...], (lanes, shares.shape[0])))

    def mix_and_sum(a):
        total = jnp.zeros((8, cols), jnp.float32)
        for piece in range(a * half, (a + 1) * half):
            took(ones.at[:, pl.ds(0, tall)], in_sem.at[piece])
            if piece == half - 1:
                for later in range(half, pieces):
                    for copy in reads(later):
                        copy.start()
                for copy in read_gains:
                    copy.start()

            def mixed(r, total):
                at = pl.ds(pl.multiple_of(piece % half * tall + r * 8, 8), 8)
                share = shares[at]
                rest = 1.0 - share
                share, rest = (jnp.concatenate([v] * (cols // lanes), axis=1) for v in (share, rest))
                fresh = share * ones[a, at] + rest * others[a, at]
                ones[a, at] = fresh
                return total + fresh * fresh

            total = lax.fori_loop(0, tall // 8, mixed, total, unroll=4)
        sums[(me, n + m)[a]] = jnp.sum(total, axis=0, keepdims=True)

    def sum_copy(source, target, recv, **device_id):
        return pltpu.make_async_remote_copy(
            src_ref=sums.at[source], dst_ref=sums.at[target],
            send_sem=sum_send.at[0], recv_sem=sum_recv.at[recv],
            device_id=device_id, device_id_type=MESH,
        )

    def exchange_up():
        took(sums.at[0], sum_recv.at[2])
        sums[n + place] = sums[n + m] + sums[n + m + 1]

        @pl.loop(1, m)
        def _(off):
            sum_copy(n + place, n + place, 1, shard=lax.rem(me + 2 * off, n)).start()

    def scales(a):
        first, count = ((0, n), (n, m))[a]
        took(sums.at[pl.ds(0, count - 1)], sum_recv.at[a])
        factors = jnp.sqrt(lax.fori_loop(1, count, lambda i, t: t + sums[first + i], sums[first]))
        (factor_gate, factor_up)[a][...] = factors
        return jnp.broadcast_to(1.0 / factors, (8, cols))

    def norm_row(off):
        return pltpu.make_async_remote_copy(
            src_ref=norm.at[mine], dst_ref=norm.at[mine],
            send_sem=norm_sem.at[0], recv_sem=norm_sem.at[1],
            device_id={"tp": lax.rem(part + off, parts)}, device_id_type=MESH,
        )

    def norm_group(off):
        return pltpu.make_async_remote_copy(
            src_ref=norm.at[pl.ds(me * parts, parts)], dst_ref=norm.at[pl.ds(me * parts, parts)],
            send_sem=norm_sem.at[0], recv_sem=norm_sem.at[2],
            device_id={"shard": lax.rem(me + off, n)}, device_id_type=MESH,
        )

    def send_early(way):
        return pltpu.make_async_remote_copy(
            src_ref=ones.at[0, pl.ds(0, ahead)], dst_ref=early.at[way],
            send_sem=early_send.at[0], recv_sem=early_recv.at[way],
            device_id=targets[way], device_id_type=MESH,
        )

    def take_early(way, j, s, scale):
        took(early.at[way], early_recv.at[way])
        for r in range(0, ahead, 8):
            there = pl.multiple_of((2 * j + s) * rows + r, 8)
            held[pl.ds(there, 8)] = (early[way, pl.ds(r, 8)] * scale).astype(jnp.bfloat16)

    def own(a):
        scale = scales(a)
        for c in range(a * half, (a + 1) * half):
            at = c % half * tall
            skip = ahead if c == 0 else 0

            def scaled(r, _):
                here = pl.multiple_of(at + r * 8, 8)
                there = pl.multiple_of((a * n + me) * rows + at + r * 8, 8)
                fresh = (ones[a, pl.ds(here, 8)] * scale).astype(jnp.bfloat16)
                held[pl.ds(there, 8)] = fresh
                if c >= min(cuts):
                    left[pl.ds(pl.multiple_of((c - min(cuts)) * tall + r * 8, 8), 8)] = fresh
                return 0

            lax.fori_loop(0, tall // 8, scaled, 0, unroll=4)
            if c < max(cuts):
                pl.when(c < line.hi)(functools.partial(line.send_own, c, skip))
            if c == (half - 1) // 2:
                exchange_up()
        return scale

    mix_and_sum(0)
    pl.semaphore_wait(barrier, n + parts - 2)

    @pl.loop(1, n)
    def _(off):
        sum_copy(me, me, 0, shard=lax.rem(me + off, n)).start()

    @pl.when(~last_place)
    def _():
        send_early(UP).start()

    @pl.when(~first_place)
    def _():
        send_early(DOWN).start()

    send_early(ACROSS).start()
    mix_and_sum(1)
    sum_copy(n + m, n + m + 1, 2, **targets[ACROSS]).start()
    scale = own(0)
    took(gains, small_sem.at[1])
    few = gains.shape[2]
    per = lanes // few
    lane = lax.broadcasted_iota(jnp.int32, (1, lanes), 1)
    summed = jnp.concatenate([gains[0] + gains[1]] * per, axis=1)
    norm[mine] = jnp.where(lane // few == mine % per, summed, 0.0)

    @pl.loop(1, parts)
    def _(off):
        norm_row(off).start()

    @pl.when(~first_place)
    def _():
        take_early(UP, place - 1, side, scale)

    @pl.when(~last_place)
    def _():
        take_early(DOWN, place + 1, side, scale)

    take_early(ACROSS, place, 1 - side, scale)
    own(1)
    took(norm.at[pl.ds(0, parts - 1)], norm_sem.at[1])

    @pl.loop(1, n)
    def _(off):
        norm_group(off).start()

    line.relay()
    took(norm.at[pl.ds(0, (n - 1) * parts)], norm_sem.at[2])

    @pl.loop(0, gain.shape[0])
    def _(r):
        gain_rows[pl.ds(r, 1)] = functools.reduce(lambda t, i: t + norm[r * per + i], range(1, per), norm[r * per])

    gain[...] = gain_rows[...].astype(jnp.bfloat16)

    line.finish()
    took(sums.at[pl.ds(0, n - 1 + m)], sum_send.at[0])
    took(norm.at[pl.ds(0, n * parts - 1)], norm_sem.at[0])

    @pl.when(first_place | last_place)
    def _():
        took(early.at[pl.ds(0, 2)], early_send.at[0])

    @pl.when(~(first_place | last_place))
    def _():
        took(early, early_send.at[0])


def rest_kernel(n, pieces, cuts, left, token, more, send_sem, recv_sem, rest_sem):
    rows = more.shape[0] // (2 * n)
    ranges = tuple((cut, pieces) for cut in cuts)
    line = Line(n, pieces, rows, ranges, left, more, send_sem, recv_sem, rest_sem, 0)
    line.greet(0)()
    pl.loop(line.lo, line.hi)(line.send_own)
    line.relay()
    line.finish()


def written(pieces, rows, cut):
    half = pieces // 2
    return [min(max(cut - a * half, 0), half) * (rows // half) for a in range(2)]


def write_kernel(
    n, pieces, cuts, held, factor_gate, factor_up, gain,
    gate, up, out_gate, out_up, out_gain, token, sem, small_sem,
):
    size = gate.shape[0]
    rows = size // n
    me = lax.axis_index("shard")
    token[...] = jnp.zeros_like(token)
    small = [
        pltpu.make_async_copy(source, out, small_sem.at[i])
        for i, (source, out) in enumerate(((factor_gate, out_gate), (factor_up, out_up), (gain, out_gain)))
    ]

    def start(a, at, count):
        at = pl.multiple_of(at, 8)
        pltpu.make_async_copy(held.at[pl.ds(a * size + at, count)], (gate, up)[a].at[pl.ds(at, count)], sem.at[0]).start()

    for turn, cut in enumerate(cuts):
        @pl.when(lax.axis_index("tp") % 2 == turn)
        def _(cut=cut):
            total = 0
            for a, count in enumerate(written(pieces, rows, cut)):
                if count:
                    pl.loop(0, n)(lambda i, a=a, count=count: start(a, i * rows, count))
                if count < rows:
                    start(a, me * rows + count, rows - count)
                total += n * count + rows - count
            for copy in small:
                copy.start()
            for copy in small:
                copy.wait()
            took(held.at[pl.ds(0, total)], sem.at[0])


def write_rest_kernel(n, pieces, cuts, more, gate_in, up_in, gate, up, sem):
    size = gate.shape[0]
    rows = size // n
    me = lax.axis_index("shard")

    def start(a, at, count):
        at = pl.multiple_of(at, 8)
        pltpu.make_async_copy(more.at[pl.ds(a * size + at, count)], (gate, up)[a].at[pl.ds(at, count)], sem.at[0]).start()

    for turn, cut in enumerate(cuts):
        @pl.when(lax.axis_index("tp") % 2 == turn)
        def _(cut=cut):
            total = 0
            for a, count in enumerate(written(pieces, rows, cut)):
                if count < rows:
                    pl.loop(1, n)(
                        lambda i, a=a, count=count: start(a, lax.rem(me + i, n) * rows + count, rows - count)
                    )
                    total += (n - 1) * (rows - count)
            took(more.at[pl.ds(0, total)], sem.at[0])


def shards(n, parts, one_gate, other_gate, one_up, other_up, mix_share, norm_train, norm_step):
    rows, cols = one_gate.shape
    few = norm_train.shape[0]
    lanes = 128
    padded = -(-rows // lanes) * lanes
    pieces = 2 * max(1, rows // 32)
    cuts = cuts_of(pieces)
    ahead = max(8, rows // 16 // 8 * 8)
    gain_shape = (n * parts * few // lanes, lanes)
    kinds = pltpu.SemaphoreType
    vmem, anywhere = pl.BlockSpec(memory_space=pltpu.VMEM), pl.BlockSpec(memory_space=pl.ANY)
    blocks = pltpu.VMEM((2 * n * rows, cols), jnp.bfloat16)
    held, left, factor_gate, factor_up, gain = pl.pallas_call(
        functools.partial(gather_kernel, n, parts, pieces, ahead, cuts),
        out_shape=(
            blocks,
            pltpu.VMEM(((pieces - min(cuts)) * rows // (pieces // 2), cols), jnp.bfloat16),
            pltpu.VMEM((1, cols), jnp.float32),
            pltpu.VMEM((1, cols), jnp.float32),
            pltpu.VMEM(gain_shape, jnp.bfloat16),
        ),
        in_specs=[pl.BlockSpec(memory_space=pltpu.HBM)] * 7,
        out_specs=(vmem,) * 5,
        scratch_shapes=[
            pltpu.VMEM((2, rows, cols), jnp.float32),
            pltpu.VMEM((2, rows, cols), jnp.float32),
            pltpu.VMEM((n + n // 2 + 2, 1, cols), jnp.float32),
            pltpu.VMEM((1, padded), jnp.float32),
            pltpu.VMEM((padded, lanes), jnp.float32),
            pltpu.VMEM((2, 1, few), jnp.float32),
            pltpu.VMEM((n * parts, 1, lanes), jnp.float32),
            pltpu.VMEM(gain_shape, jnp.float32),
            pltpu.VMEM((3, ahead, cols), jnp.float32),
            kinds.DMA((1,)),
            kinds.DMA((3,)),
            kinds.DMA((pieces,)),
            kinds.DMA((2,)),
            kinds.DMA((1,)),
            kinds.DMA((3,)),
            kinds.DMA((3,)),
            kinds.DMA((3,)),
            kinds.DMA((n // 2, max(cuts))),
            kinds.DMA((1,)),
        ],
        compiler_params=pltpu.CompilerParams(
            collective_id=0, has_side_effects=True, vmem_limit_bytes=46 * 2**20
        ),
        name="mix_gather",
    )(
        one_gate, other_gate, one_up, other_up,
        jnp.pad(mix_share, (0, padded - rows))[None], norm_train[None], norm_step[None],
    )
    small = pltpu.CompilerParams(vmem_limit_bytes=2**20)
    whole = (jax.ShapeDtypeStruct((n * rows, cols), jnp.bfloat16),) * 2
    gate, up, factor_gate, factor_up, gain, token = pl.pallas_call(
        functools.partial(write_kernel, n, pieces, cuts),
        out_shape=whole + (jax.ShapeDtypeStruct((1, cols), jnp.float32),) * 2
        + (jax.ShapeDtypeStruct(gain_shape, jnp.bfloat16), pltpu.VMEM((8, lanes), jnp.float32)),
        in_specs=[vmem] * 4,
        out_specs=(anywhere,) * 5 + (vmem,),
        scratch_shapes=[kinds.DMA((1,)), kinds.DMA((3,))],
        compiler_params=small,
        name="write_out",
    )(held, factor_gate, factor_up, gain)
    more = pl.pallas_call(
        functools.partial(rest_kernel, n, pieces, cuts),
        out_shape=blocks,
        in_specs=[vmem] * 2,
        out_specs=vmem,
        scratch_shapes=[kinds.DMA((3,)), kinds.DMA((n // 2, pieces - min(cuts))), kinds.DMA((1,))],
        compiler_params=pltpu.CompilerParams(collective_id=1, has_side_effects=True, vmem_limit_bytes=2**20),
        name="gather_rest",
    )(left, token)
    gate, up = pl.pallas_call(
        functools.partial(write_rest_kernel, n, pieces, cuts),
        out_shape=whole,
        in_specs=[vmem, anywhere, anywhere],
        out_specs=(anywhere,) * 2,
        input_output_aliases={1: 0, 2: 1},
        scratch_shapes=[kinds.DMA((1,))],
        compiler_params=small,
        name="write_rest",
    )(more, gate, up)
    return gate, up, factor_gate[0], factor_up[0], gain.reshape(-1)


def solution(mesh):
    return jax.shard_map(
        functools.partial(shards, mesh.shape["shard"], mesh.shape["tp"]),
        mesh=mesh,
        in_specs=(
            P("shard", "tp"),
            P("shard", "tp"),
            P("shard", "tp"),
            P("shard", "tp"),
            P("shard"),
            P(("shard", "tp")),
            P(("shard", "tp")),
        ),
        out_specs=(P(None, "tp"), P(None, "tp"), P("tp"), P("tp"), P()),
        check_vma=False,
    )
```

```python
import functools

import jax
import jax.numpy as jnp
import numpy as np
from jax import lax
from jax.experimental import pallas as pl
from jax.experimental.pallas import tpu as pltpu
from jax.sharding import PartitionSpec as P

MESH = pl.DeviceIdType.MESH
UP, DOWN, ACROSS = 0, 1, 2
CUTS = (12, 15)


def crosses(place, m, j, c):
    last = m - 1
    kept = ((place == 0) & (j == 1)) | ((place == last) & (j == last - 1))
    kept = kept & (c % 2 == 1)
    return ~(kept | ((place == 1) & (j == 0)) | ((place == last - 1) & (j == last)))


def sent(m, lo, hi, place):
    last, count = m - 1, hi - lo
    extra = count if place in (0, last) else 0
    inner = sum(c % 2 for c in range(lo, hi)) if place in (1, last - 1) else 0
    up = (place + 1) * count * (place != last) + extra * (place == 0) + inner * (place == last - 1)
    down = (m - place) * count * (place != 0) + extra * (place == last) + inner * (place == 1)
    across = count + sum(
        bool(crosses(np.int64(place), m, np.int64(j), np.int64(c)))
        for j in range(m) if j != place for c in range(lo, hi)
    )
    return up, down, across


def cuts_of(pieces):
    return tuple(min(max(1, pieces * cut // 16), pieces - 1) for cut in CUTS)


def took(ref, sem):
    pltpu.make_async_copy(ref, ref, sem).wait()


class Line:
    def __init__(self, n, pieces, rows, ranges, own, land, send_sem, recv_sem, rest_sem, ahead):
        self.n, self.m, self.half = n, n // 2, pieces // 2
        self.rows, self.tall, self.ranges, self.ahead = rows, rows // (pieces // 2), ranges, ahead
        self.me = lax.axis_index("shard")
        self.place, self.side = self.me // 2, self.me % 2
        self.turn = lax.axis_index("tp") % 2
        self.lo, self.hi = (jnp.where(self.turn == 0, first, second) for first, second in zip(*ranges))
        self.base = min(lo for lo, _ in ranges)
        self.own, self.land = own, land
        self.send_sem, self.recv_sem, self.rest_sem = send_sem, recv_sem, rest_sem
        self.first, self.last = self.place == 0, self.place == self.m - 1
        me = self.me
        self.targets = {
            UP: {"shard": lax.rem(me + 2, n)},
            DOWN: {"shard": lax.rem(me + n - 2, n)},
            ACROSS: {"shard": 2 * self.place + 1 - self.side},
        }

    def greet(self, others):
        barrier = pltpu.get_barrier_semaphore()
        for way, unless in ((UP, self.last), (DOWN, self.first), (ACROSS, self.place < 0)):
            @pl.when(~unless)
            def _(way=way):
                pl.semaphore_signal(barrier, inc=1, device_id=self.targets[way], device_id_type=MESH)

        ends = self.first | self.last

        def wait():
            @pl.when(ends)
            def _():
                pl.semaphore_wait(barrier, 2 + others)

            @pl.when(~ends)
            def _():
                pl.semaphore_wait(barrier, 3 + others)

        return wait

    def piece(self, ref, j, s, c, skip=0):
        at = (c // self.half * self.n + 2 * j + s) * self.rows + c % self.half * self.tall + skip
        return ref.at[pl.ds(pl.multiple_of(at, 8), self.tall - skip)]

    def send(self, way, j, s, c, rest=False, skip=0, own=False):
        own = own and self.own is not None
        source = self.own.at[pl.ds(pl.multiple_of((c - self.base) * self.tall, 8), self.tall)] if own else None
        return pltpu.make_async_remote_copy(
            src_ref=self.piece(self.land, j, s, c, skip) if source is None else source,
            dst_ref=self.piece(self.land, j, s, c, skip),
            send_sem=self.send_sem.at[way],
            recv_sem=self.rest_sem.at[0] if rest else self.recv_sem.at[j, c - self.base],
            device_id=self.targets[way], device_id_type=MESH,
        )

    def send_own(self, c, skip=0):
        @pl.when(~self.last)
        def _():
            self.send(UP, self.place, self.side, c, False, skip, True).start()

        @pl.when(~self.first)
        def _():
            self.send(DOWN, self.place, self.side, c, False, skip, True).start()

        self.send(ACROSS, self.place, self.side, c, False, skip, True).start()

    def arrived(self, j, s, c, first):
        def whole():
            took(self.piece(self.land, j, s, c), self.recv_sem.at[j, c - self.base])

        if not self.ahead:
            return whole()

        @pl.when(first)
        def _():
            took(self.piece(self.land, j, s, c, self.ahead), self.recv_sem.at[j, c - self.base])

        pl.when(~first)(whole)

    def relay(self):
        place, side, m, last = self.place, self.side, self.m, self.m - 1
        ends, inner = self.first | self.last, (place == 1) | (place == last - 1)

        @pl.loop(0, last)
        def _(b):
            @pl.loop(self.lo, self.hi)
            def _(c):
                def pass_on(way, j, stop):
                    self.arrived(j, side, c, (b == 0) & (c == 0))

                    @pl.when(~stop)
                    def _():
                        self.send(way, j, side, c).start()

                    @pl.when(crosses(place, m, j, c))
                    def _():
                        self.send(ACROSS, j, side, c, True).start()

                @pl.when(b < place)
                def _():
                    pass_on(UP, place - 1 - b, self.last)

                @pl.when(b < last - place)
                def _():
                    pass_on(DOWN, place + 1 + b, self.first)

                @pl.when((ends & (b == 1)) | (inner & (b == last - 1) & (c % 2 == 1)))
                def _():
                    self.arrived(place, 1 - side, c, c == 0)

                    @pl.when(self.first | (place == last - 1))
                    def _():
                        self.send(UP, place, 1 - side, c, True).start()

                    @pl.when(self.last | (place == 1))
                    def _():
                        self.send(DOWN, place, 1 - side, c, True).start()

    def finish(self):
        place, side, last = self.place, self.side, self.m - 1
        ends, inner = self.first | self.last, (place == 1) | (place == last - 1)

        @pl.loop(self.lo, self.hi)
        def _(c):
            @pl.when(~(ends | (inner & (c % 2 == 1))))
            def _():
                self.arrived(place, 1 - side, c, c == 0)

        for turn, (lo, hi) in enumerate(self.ranges):
            @pl.when(self.turn == turn)
            def _(lo=lo, hi=hi):
                took(self.land.at[pl.ds(0, last * (hi - lo) * self.tall)], self.rest_sem.at[0])
                for k in range(self.m):
                    @pl.when(place == k)
                    def _(k=k):
                        for way, count in enumerate(sent(self.m, lo, hi, k)):
                            if count:
                                took(self.land.at[pl.ds(0, count * self.tall - self.ahead)], self.send_sem.at[way])


def gather_kernel(
    n, parts, pieces, ahead, cuts, one_gate, other_gate, one_up, other_up, mix, train, step,
    held, left, factor_gate, factor_up, gain,
    ones, others, sums, mix_row, shares, gains, norm, gain_rows, early,
    early_send, early_recv, in_sem, small_sem, sum_send, sum_recv, norm_sem, send_sem, recv_sem, rest_sem,
):
    me = lax.axis_index("shard")
    part = lax.axis_index("tp")
    m, half = n // 2, pieces // 2
    place, side = me // 2, me % 2
    rows, cols = ones.shape[1:]
    tall = rows // half
    mine = me * parts + part
    ranges = tuple((0, cut) for cut in cuts)
    line = Line(n, pieces, rows, ranges, None, held, send_sem, recv_sem, rest_sem, ahead)
    targets, first_place, last_place = line.targets, line.first, line.last
    lanes = shares.shape[1]

    read_mix = pltpu.make_async_copy(mix, mix_row, small_sem.at[0])
    read_mix.start()
    barrier = pltpu.get_barrier_semaphore()

    @pl.loop(1, n)
    def _(off):
        pl.semaphore_signal(barrier, inc=1, device_id={"shard": lax.rem(me + off, n)}, device_id_type=MESH)

    @pl.loop(1, parts)
    def _(off):
        pl.semaphore_signal(barrier, inc=1, device_id={"tp": lax.rem(part + off, parts)}, device_id_type=MESH)

    read_gains = [
        pltpu.make_async_copy(source, gains.at[i], small_sem.at[1]) for i, source in enumerate((train, step))
    ]

    def reads(piece):
        a, at = piece // half, pl.ds(piece % half * tall, tall)
        first, second = ((one_gate, other_gate), (one_up, other_up))[a]
        return (
            pltpu.make_async_copy(first.at[at], ones.at[a, at], in_sem.at[piece]),
            pltpu.make_async_copy(second.at[at], others.at[a, at], in_sem.at[piece]),
        )

    for piece in range(half):
        for copy in reads(piece):
            copy.start()
    read_mix.wait()
    shares[...] = jnp.transpose(jnp.broadcast_to(mix_row[...], (lanes, shares.shape[0])))

    def mix_and_sum(a):
        total = jnp.zeros((8, cols), jnp.float32)
        for piece in range(a * half, (a + 1) * half):
            took(ones.at[:, pl.ds(0, tall)], in_sem.at[piece])
            if piece == half - 1:
                for later in range(half, pieces):
                    for copy in reads(later):
                        copy.start()
                for copy in read_gains:
                    copy.start()

            def mixed(r, total):
                at = pl.ds(pl.multiple_of(piece % half * tall + r * 8, 8), 8)
                share = shares[at]
                rest = 1.0 - share
                share, rest = (jnp.concatenate([v] * (cols // lanes), axis=1) for v in (share, rest))
                fresh = share * ones[a, at] + rest * others[a, at]
                ones[a, at] = fresh
                return total + fresh * fresh

            total = lax.fori_loop(0, tall // 8, mixed, total, unroll=4)
        sums[(me, n + m)[a]] = jnp.sum(total, axis=0, keepdims=True)

    def sum_copy(source, target, recv, **device_id):
        return pltpu.make_async_remote_copy(
            src_ref=sums.at[source], dst_ref=sums.at[target],
            send_sem=sum_send.at[0], recv_sem=sum_recv.at[recv],
            device_id=device_id, device_id_type=MESH,
        )

    def exchange_up():
        took(sums.at[0], sum_recv.at[2])
        sums[n + place] = sums[n + m] + sums[n + m + 1]

        @pl.loop(1, m)
        def _(off):
            sum_copy(n + place, n + place, 1, shard=lax.rem(me + 2 * off, n)).start()

    def scales(a):
        first, count = ((0, n), (n, m))[a]
        took(sums.at[pl.ds(0, count - 1)], sum_recv.at[a])
        factors = jnp.sqrt(lax.fori_loop(1, count, lambda i, t: t + sums[first + i], sums[first]))
        (factor_gate, factor_up)[a][...] = factors
        return jnp.broadcast_to(1.0 / factors, (8, cols))

    def norm_row(off):
        return pltpu.make_async_remote_copy(
            src_ref=norm.at[mine], dst_ref=norm.at[mine],
            send_sem=norm_sem.at[0], recv_sem=norm_sem.at[1],
            device_id={"tp": lax.rem(part + off, parts)}, device_id_type=MESH,
        )

    def norm_group(off):
        return pltpu.make_async_remote_copy(
            src_ref=norm.at[pl.ds(me * parts, parts)], dst_ref=norm.at[pl.ds(me * parts, parts)],
            send_sem=norm_sem.at[0], recv_sem=norm_sem.at[2],
            device_id={"shard": lax.rem(me + off, n)}, device_id_type=MESH,
        )

    def send_early(way):
        return pltpu.make_async_remote_copy(
            src_ref=ones.at[0, pl.ds(0, ahead)], dst_ref=early.at[way],
            send_sem=early_send.at[0], recv_sem=early_recv.at[way],
            device_id=targets[way], device_id_type=MESH,
        )

    def take_early(way, j, s, scale):
        took(early.at[way], early_recv.at[way])
        for r in range(0, ahead, 8):
            there = pl.multiple_of((2 * j + s) * rows + r, 8)
            held[pl.ds(there, 8)] = (early[way, pl.ds(r, 8)] * scale).astype(jnp.bfloat16)

    def own(a):
        scale = scales(a)
        for c in range(a * half, (a + 1) * half):
            at = c % half * tall
            skip = ahead if c == 0 else 0

            def scaled(r, _):
                here = pl.multiple_of(at + r * 8, 8)
                there = pl.multiple_of((a * n + me) * rows + at + r * 8, 8)
                fresh = (ones[a, pl.ds(here, 8)] * scale).astype(jnp.bfloat16)
                held[pl.ds(there, 8)] = fresh
                if c >= min(cuts):
                    left[pl.ds(pl.multiple_of((c - min(cuts)) * tall + r * 8, 8), 8)] = fresh
                return 0

            lax.fori_loop(0, tall // 8, scaled, 0, unroll=4)
            if c < max(cuts):
                pl.when(c < line.hi)(functools.partial(line.send_own, c, skip))
            if c == (half - 1) // 2:
                exchange_up()
        return scale

    mix_and_sum(0)
    pl.semaphore_wait(barrier, n + parts - 2)

    @pl.loop(1, n)
    def _(off):
        sum_copy(me, me, 0, shard=lax.rem(me + off, n)).start()

    @pl.when(~last_place)
    def _():
        send_early(UP).start()

    @pl.when(~first_place)
    def _():
        send_early(DOWN).start()

    send_early(ACROSS).start()
    mix_and_sum(1)
    sum_copy(n + m, n + m + 1, 2, **targets[ACROSS]).start()
    scale = own(0)
    took(gains, small_sem.at[1])
    few = gains.shape[2]
    per = lanes // few
    lane = lax.broadcasted_iota(jnp.int32, (1, lanes), 1)
    summed = jnp.concatenate([gains[0] + gains[1]] * per, axis=1)
    norm[mine] = jnp.where(lane // few == mine % per, summed, 0.0)

    @pl.loop(1, parts)
    def _(off):
        norm_row(off).start()

    @pl.when(~first_place)
    def _():
        take_early(UP, place - 1, side, scale)

    @pl.when(~last_place)
    def _():
        take_early(DOWN, place + 1, side, scale)

    take_early(ACROSS, place, 1 - side, scale)
    own(1)
    took(norm.at[pl.ds(0, parts - 1)], norm_sem.at[1])

    @pl.loop(1, n)
    def _(off):
        norm_group(off).start()

    line.relay()
    took(norm.at[pl.ds(0, (n - 1) * parts)], norm_sem.at[2])

    @pl.loop(0, gain.shape[0])
    def _(r):
        gain_rows[pl.ds(r, 1)] = functools.reduce(lambda t, i: t + norm[r * per + i], range(1, per), norm[r * per])

    gain[...] = gain_rows[...].astype(jnp.bfloat16)

    line.finish()
    took(sums.at[pl.ds(0, n - 1 + m)], sum_send.at[0])
    took(norm.at[pl.ds(0, n * parts - 1)], norm_sem.at[0])

    @pl.when(first_place | last_place)
    def _():
        took(early.at[pl.ds(0, 2)], early_send.at[0])

    @pl.when(~(first_place | last_place))
    def _():
        took(early, early_send.at[0])


def rest_kernel(n, pieces, cuts, left, token, more, send_sem, recv_sem, rest_sem):
    rows = more.shape[0] // (2 * n)
    ranges = tuple((cut, pieces) for cut in cuts)
    line = Line(n, pieces, rows, ranges, left, more, send_sem, recv_sem, rest_sem, 0)
    line.greet(0)()
    pl.loop(line.lo, line.hi)(line.send_own)
    line.relay()
    line.finish()


def written(pieces, rows, cut):
    half = pieces // 2
    return [min(max(cut - a * half, 0), half) * (rows // half) for a in range(2)]


def write_kernel(
    n, pieces, cuts, held, factor_gate, factor_up, gain,
    gate, up, out_gate, out_up, out_gain, token, sem, small_sem,
):
    size = gate.shape[0]
    rows = size // n
    me = lax.axis_index("shard")
    token[...] = jnp.zeros_like(token)
    small = [
        pltpu.make_async_copy(source, out, small_sem.at[i])
        for i, (source, out) in enumerate(((factor_gate, out_gate), (factor_up, out_up), (gain, out_gain)))
    ]

    def start(a, at, count):
        at = pl.multiple_of(at, 8)
        pltpu.make_async_copy(held.at[pl.ds(a * size + at, count)], (gate, up)[a].at[pl.ds(at, count)], sem.at[0]).start()

    for turn, cut in enumerate(cuts):
        @pl.when(lax.axis_index("tp") % 2 == turn)
        def _(cut=cut):
            total = 0
            for a, count in enumerate(written(pieces, rows, cut)):
                if count:
                    pl.loop(0, n)(lambda i, a=a, count=count: start(a, i * rows, count))
                if count < rows:
                    start(a, me * rows + count, rows - count)
                total += n * count + rows - count
            for copy in small:
                copy.start()
            for copy in small:
                copy.wait()
            took(held.at[pl.ds(0, total)], sem.at[0])


def write_rest_kernel(n, pieces, cuts, more, gate_in, up_in, gate, up, sem):
    size = gate.shape[0]
    rows = size // n
    me = lax.axis_index("shard")

    def start(a, at, count):
        at = pl.multiple_of(at, 8)
        pltpu.make_async_copy(more.at[pl.ds(a * size + at, count)], (gate, up)[a].at[pl.ds(at, count)], sem.at[0]).start()

    for turn, cut in enumerate(cuts):
        @pl.when(lax.axis_index("tp") % 2 == turn)
        def _(cut=cut):
            total = 0
            for a, count in enumerate(written(pieces, rows, cut)):
                if count < rows:
                    pl.loop(1, n)(
                        lambda i, a=a, count=count: start(a, lax.rem(me + i, n) * rows + count, rows - count)
                    )
                    total += (n - 1) * (rows - count)
            took(more.at[pl.ds(0, total)], sem.at[0])


def shards(n, parts, one_gate, other_gate, one_up, other_up, mix_share, norm_train, norm_step):
    rows, cols = one_gate.shape
    few = norm_train.shape[0]
    lanes = 128
    padded = -(-rows // lanes) * lanes
    pieces = 2 * max(1, rows // 32)
    cuts = cuts_of(pieces)
    ahead = max(8, rows // 16 // 8 * 8)
    gain_shape = (n * parts * few // lanes, lanes)
    kinds = pltpu.SemaphoreType
    vmem, anywhere = pl.BlockSpec(memory_space=pltpu.VMEM), pl.BlockSpec(memory_space=pl.ANY)
    blocks = pltpu.VMEM((2 * n * rows, cols), jnp.bfloat16)
    held, left, factor_gate, factor_up, gain = pl.pallas_call(
        functools.partial(gather_kernel, n, parts, pieces, ahead, cuts),
        out_shape=(
            blocks,
            pltpu.VMEM(((pieces - min(cuts)) * rows // (pieces // 2), cols), jnp.bfloat16),
            pltpu.VMEM((1, cols), jnp.float32),
            pltpu.VMEM((1, cols), jnp.float32),
            pltpu.VMEM(gain_shape, jnp.bfloat16),
        ),
        in_specs=[pl.BlockSpec(memory_space=pltpu.HBM)] * 7,
        out_specs=(vmem,) * 5,
        scratch_shapes=[
            pltpu.VMEM((2, rows, cols), jnp.float32),
            pltpu.VMEM((2, rows, cols), jnp.float32),
            pltpu.VMEM((n + n // 2 + 2, 1, cols), jnp.float32),
            pltpu.VMEM((1, padded), jnp.float32),
            pltpu.VMEM((padded, lanes), jnp.float32),
            pltpu.VMEM((2, 1, few), jnp.float32),
            pltpu.VMEM((n * parts, 1, lanes), jnp.float32),
            pltpu.VMEM(gain_shape, jnp.float32),
            pltpu.VMEM((3, ahead, cols), jnp.float32),
            kinds.DMA((1,)),
            kinds.DMA((3,)),
            kinds.DMA((pieces,)),
            kinds.DMA((2,)),
            kinds.DMA((1,)),
            kinds.DMA((3,)),
            kinds.DMA((3,)),
            kinds.DMA((3,)),
            kinds.DMA((n // 2, max(cuts))),
            kinds.DMA((1,)),
        ],
        compiler_params=pltpu.CompilerParams(
            collective_id=0, has_side_effects=True, vmem_limit_bytes=46 * 2**20
        ),
        name="mix_gather",
    )(
        one_gate, other_gate, one_up, other_up,
        jnp.pad(mix_share, (0, padded - rows))[None], norm_train[None], norm_step[None],
    )
    small = pltpu.CompilerParams(vmem_limit_bytes=2**20)
    whole = (jax.ShapeDtypeStruct((n * rows, cols), jnp.bfloat16),) * 2
    gate, up, factor_gate, factor_up, gain, token = pl.pallas_call(
        functools.partial(write_kernel, n, pieces, cuts),
        out_shape=whole + (jax.ShapeDtypeStruct((1, cols), jnp.float32),) * 2
        + (jax.ShapeDtypeStruct(gain_shape, jnp.bfloat16), pltpu.VMEM((8, lanes), jnp.float32)),
        in_specs=[vmem] * 4,
        out_specs=(anywhere,) * 5 + (vmem,),
        scratch_shapes=[kinds.DMA((1,)), kinds.DMA((3,))],
        compiler_params=small,
        name="write_out",
    )(held, factor_gate, factor_up, gain)
    more = pl.pallas_call(
        functools.partial(rest_kernel, n, pieces, cuts),
        out_shape=blocks,
        in_specs=[vmem] * 2,
        out_specs=vmem,
        scratch_shapes=[kinds.DMA((3,)), kinds.DMA((n // 2, pieces - min(cuts))), kinds.DMA((1,))],
        compiler_params=pltpu.CompilerParams(collective_id=1, has_side_effects=True, vmem_limit_bytes=2**20),
        name="gather_rest",
    )(left, token)
    gate, up = pl.pallas_call(
        functools.partial(write_rest_kernel, n, pieces, cuts),
        out_shape=whole,
        in_specs=[vmem, anywhere, anywhere],
        out_specs=(anywhere,) * 2,
        input_output_aliases={1: 0, 2: 1},
        scratch_shapes=[kinds.DMA((1,))],
        compiler_params=small,
        name="write_rest",
    )(more, gate, up)
    return gate, up, factor_gate[0], factor_up[0], gain.reshape(-1)


def solution(mesh):
    return jax.shard_map(
        functools.partial(shards, mesh.shape["shard"], mesh.shape["tp"]),
        mesh=mesh,
        in_specs=(
            P("shard", "tp"),
            P("shard", "tp"),
            P("shard", "tp"),
            P("shard", "tp"),
            P("shard"),
            P(("shard", "tp")),
            P(("shard", "tp")),
        ),
        out_specs=(P(None, "tp"), P(None, "tp"), P("tp"), P("tp"), P()),
        check_vma=False,
    )
```

```python
import functools

import jax
import jax.numpy as jnp
import numpy as np
from jax import lax
from jax.experimental import pallas as pl
from jax.experimental.pallas import tpu as pltpu
from jax.sharding import PartitionSpec as P

MESH = pl.DeviceIdType.MESH
UP, DOWN, ACROSS = 0, 1, 2
LATE = ((1, 1), (8, 8))


def crosses(place, m, j, c):
    last = m - 1
    kept = ((place == 0) & (j == 1)) | ((place == last) & (j == last - 1))
    kept = kept & (c % 2 == 1)
    return ~(kept | ((place == 1) & (j == 0)) | ((place == last - 1) & (j == last)))


def sent(m, pieces, late, place):
    last, count = m - 1, pieces
    extra = count if place in (0, last) else 0
    inner = pieces // 2 if place in (1, last - 1) else 0
    up = (place + 1) * count * (place != last) + extra * (place == 0) + inner * (place == last - 1)
    down = (m - place) * count * (place != 0) + extra * (place == last) + inner * (place == 1)
    across = count + sum(
        bool(crosses(np.int64(place), m, np.int64(j), np.int64(c)))
        for j in range(m) if j != place for c in range(pieces)
    )
    return up - late[0] * (place == last - 1), down - late[0] * (place == 1), across - late[1] * (place in (0, last))


def late_of(pieces):
    return tuple((min(along, pieces // 2), min(across, pieces - 1)) for along, across in LATE)


def took(ref, sem):
    pltpu.make_async_copy(ref, ref, sem).wait()


class Line:
    def __init__(self, n, pieces, rows, lates, land, send_sem, recv_sem, rest_sem, ahead):
        self.n, self.m, self.half = n, n // 2, pieces // 2
        self.rows, self.tall, self.pieces, self.lates, self.ahead = rows, rows // (pieces // 2), pieces, lates, ahead
        self.me = lax.axis_index("shard")
        self.place, self.side = self.me // 2, self.me % 2
        self.turn = lax.axis_index("tp") % 2
        self.along, self.across = (jnp.where(self.turn == 0, *counts) for counts in zip(*lates))
        self.land = land
        self.send_sem, self.recv_sem, self.rest_sem = send_sem, recv_sem, rest_sem
        self.first, self.last = self.place == 0, self.place == self.m - 1
        me = self.me
        self.targets = {
            UP: {"shard": lax.rem(me + 2, n)},
            DOWN: {"shard": lax.rem(me + n - 2, n)},
            ACROSS: {"shard": 2 * self.place + 1 - self.side},
        }

    def late_along(self, c):
        return (c % 2 == 1) & (c >= self.pieces - 2 * self.along)

    def late_across(self, j, c):
        far = jnp.where(self.first, self.m - 1, 0)
        return (self.first | self.last) & (j == far) & (c >= self.pieces - self.across)

    def piece(self, ref, j, s, c, skip=0):
        at = (c // self.half * self.n + 2 * j + s) * self.rows + c % self.half * self.tall + skip
        return ref.at[pl.ds(pl.multiple_of(at, 8), self.tall - skip)]

    def send(self, way, j, s, c, rest=False, skip=0):
        block = self.piece(self.land, j, s, c, skip)
        return pltpu.make_async_remote_copy(
            src_ref=block, dst_ref=block,
            send_sem=self.send_sem.at[way], recv_sem=self.rest_sem.at[0] if rest else self.recv_sem.at[j, c],
            device_id=self.targets[way], device_id_type=MESH,
        )

    def send_own(self, c, skip=0):
        late = self.late_along(c)

        @pl.when(~(self.last | ((self.place == self.m - 2) & late)))
        def _():
            self.send(UP, self.place, self.side, c, False, skip).start()

        @pl.when(~(self.first | ((self.place == 1) & late)))
        def _():
            self.send(DOWN, self.place, self.side, c, False, skip).start()

        self.send(ACROSS, self.place, self.side, c, False, skip).start()

    def arrived(self, j, s, c, first):
        def whole():
            took(self.piece(self.land, j, s, c), self.recv_sem.at[j, c])

        if not self.ahead:
            return whole()

        @pl.when(first)
        def _():
            took(self.piece(self.land, j, s, c, self.ahead), self.recv_sem.at[j, c])

        pl.when(~first)(whole)

    def relay(self):
        place, side, m, last = self.place, self.side, self.m, self.m - 1
        ends, inner = self.first | self.last, (place == 1) | (place == last - 1)

        @pl.loop(0, last)
        def _(b):
            @pl.loop(0, self.pieces)
            def _(c):
                late = self.late_along(c) & (b == 0)

                def pass_on(way, j, stop):
                    self.arrived(j, side, c, (b == 0) & (c == 0))

                    @pl.when(~stop)
                    def _():
                        self.send(way, j, side, c).start()

                    @pl.when(crosses(place, m, j, c) & ~self.late_across(j, c))
                    def _():
                        self.send(ACROSS, j, side, c, True).start()

                @pl.when((b < place) & ~(self.last & late))
                def _():
                    pass_on(UP, place - 1 - b, self.last)

                @pl.when((b < last - place) & ~(self.first & late))
                def _():
                    pass_on(DOWN, place + 1 + b, self.first)

                @pl.when((ends & (b == 1)) | (inner & (b == last - 1) & (c % 2 == 1)))
                def _():
                    self.arrived(place, 1 - side, c, c == 0)

                    @pl.when(self.first | (place == last - 1))
                    def _():
                        self.send(UP, place, 1 - side, c, True).start()

                    @pl.when(self.last | (place == 1))
                    def _():
                        self.send(DOWN, place, 1 - side, c, True).start()

    def finish(self):
        place, side, last = self.place, self.side, self.m - 1
        ends, inner = self.first | self.last, (place == 1) | (place == last - 1)

        @pl.loop(0, self.pieces)
        def _(c):
            @pl.when(~(ends | (inner & (c % 2 == 1))))
            def _():
                self.arrived(place, 1 - side, c, c == 0)

        for turn, late in enumerate(self.lates):
            for k in range(self.m):
                @pl.when((self.turn == turn) & (place == k))
                def _(late=late, k=k):
                    rest = last * self.pieces - late[1] * (k in (0, last))
                    took(self.land.at[pl.ds(0, rest * self.tall)], self.rest_sem.at[0])
                    for way, count in enumerate(sent(self.m, self.pieces, late, k)):
                        if count:
                            took(self.land.at[pl.ds(0, count * self.tall - self.ahead)], self.send_sem.at[way])


def gather_kernel(
    n, parts, pieces, ahead, lates, one_gate, other_gate, one_up, other_up, mix, train, step,
    held, left, factor_gate, factor_up, gain,
    ones, others, sums, mix_row, shares, gains, norm, gain_rows, early,
    early_send, early_recv, in_sem, small_sem, sum_send, sum_recv, norm_sem, send_sem, recv_sem, rest_sem,
):
    me = lax.axis_index("shard")
    part = lax.axis_index("tp")
    m, half = n // 2, pieces // 2
    place, side = me // 2, me % 2
    rows, cols = ones.shape[1:]
    tall = rows // half
    mine = me * parts + part
    line = Line(n, pieces, rows, lates, held, send_sem, recv_sem, rest_sem, ahead)
    targets, first_place, last_place = line.targets, line.first, line.last
    lanes = shares.shape[1]

    read_mix = pltpu.make_async_copy(mix, mix_row, small_sem.at[0])
    read_mix.start()
    barrier = pltpu.get_barrier_semaphore()

    @pl.loop(1, n)
    def _(off):
        pl.semaphore_signal(barrier, inc=1, device_id={"shard": lax.rem(me + off, n)}, device_id_type=MESH)

    @pl.loop(1, parts)
    def _(off):
        pl.semaphore_signal(barrier, inc=1, device_id={"tp": lax.rem(part + off, parts)}, device_id_type=MESH)

    read_gains = [
        pltpu.make_async_copy(source, gains.at[i], small_sem.at[1]) for i, source in enumerate((train, step))
    ]

    def reads(piece):
        a, at = piece // half, pl.ds(piece % half * tall, tall)
        first, second = ((one_gate, other_gate), (one_up, other_up))[a]
        return (
            pltpu.make_async_copy(first.at[at], ones.at[a, at], in_sem.at[piece]),
            pltpu.make_async_copy(second.at[at], others.at[a, at], in_sem.at[piece]),
        )

    for piece in range(half):
        for copy in reads(piece):
            copy.start()
    read_mix.wait()
    shares[...] = jnp.transpose(jnp.broadcast_to(mix_row[...], (lanes, shares.shape[0])))

    def mix_and_sum(a):
        total = jnp.zeros((8, cols), jnp.float32)
        for piece in range(a * half, (a + 1) * half):
            took(ones.at[:, pl.ds(0, tall)], in_sem.at[piece])
            if piece == half - 1:
                for later in range(half, pieces):
                    for copy in reads(later):
                        copy.start()
                for copy in read_gains:
                    copy.start()

            def mixed(r, total):
                at = pl.ds(pl.multiple_of(piece % half * tall + r * 8, 8), 8)
                share = shares[at]
                rest = 1.0 - share
                share, rest = (jnp.concatenate([v] * (cols // lanes), axis=1) for v in (share, rest))
                fresh = share * ones[a, at] + rest * others[a, at]
                ones[a, at] = fresh
                return total + fresh * fresh

            total = lax.fori_loop(0, tall // 8, mixed, total, unroll=4)
        sums[(me, n + m)[a]] = jnp.sum(total, axis=0, keepdims=True)

    def sum_copy(source, target, recv, **device_id):
        return pltpu.make_async_remote_copy(
            src_ref=sums.at[source], dst_ref=sums.at[target],
            send_sem=sum_send.at[0], recv_sem=sum_recv.at[recv],
            device_id=device_id, device_id_type=MESH,
        )

    def exchange_up():
        took(sums.at[0], sum_recv.at[2])
        sums[n + place] = sums[n + m] + sums[n + m + 1]

        @pl.loop(1, m)
        def _(off):
            sum_copy(n + place, n + place, 1, shard=lax.rem(me + 2 * off, n)).start()

    def scales(a):
        first, count = ((0, n), (n, m))[a]
        took(sums.at[pl.ds(0, count - 1)], sum_recv.at[a])
        factors = jnp.sqrt(lax.fori_loop(1, count, lambda i, t: t + sums[first + i], sums[first]))
        (factor_gate, factor_up)[a][...] = factors
        return jnp.broadcast_to(1.0 / factors, (8, cols))

    def norm_row(off):
        return pltpu.make_async_remote_copy(
            src_ref=norm.at[mine], dst_ref=norm.at[mine],
            send_sem=norm_sem.at[0], recv_sem=norm_sem.at[1],
            device_id={"tp": lax.rem(part + off, parts)}, device_id_type=MESH,
        )

    def norm_group(off):
        return pltpu.make_async_remote_copy(
            src_ref=norm.at[pl.ds(me * parts, parts)], dst_ref=norm.at[pl.ds(me * parts, parts)],
            send_sem=norm_sem.at[0], recv_sem=norm_sem.at[2],
            device_id={"shard": lax.rem(me + off, n)}, device_id_type=MESH,
        )

    def send_early(way):
        return pltpu.make_async_remote_copy(
            src_ref=ones.at[0, pl.ds(0, ahead)], dst_ref=early.at[way],
            send_sem=early_send.at[0], recv_sem=early_recv.at[way],
            device_id=targets[way], device_id_type=MESH,
        )

    def take_early(way, j, s, scale):
        took(early.at[way], early_recv.at[way])
        for r in range(0, ahead, 8):
            there = pl.multiple_of((2 * j + s) * rows + r, 8)
            held[pl.ds(there, 8)] = (early[way, pl.ds(r, 8)] * scale).astype(jnp.bfloat16)

    def own(a):
        scale = scales(a)
        for c in range(a * half, (a + 1) * half):
            at = c % half * tall
            skip = ahead if c == 0 else 0

            def scaled(r, _):
                here = pl.multiple_of(at + r * 8, 8)
                there = pl.multiple_of((a * n + me) * rows + at + r * 8, 8)
                held[pl.ds(there, 8)] = (ones[a, pl.ds(here, 8)] * scale).astype(jnp.bfloat16)
                return 0

            lax.fori_loop(0, tall // 8, scaled, 0, unroll=4)
            line.send_own(c, skip)
            if c == (half - 1) // 2:
                exchange_up()
        return scale

    mix_and_sum(0)
    pl.semaphore_wait(barrier, n + parts - 2)

    @pl.loop(1, n)
    def _(off):
        sum_copy(me, me, 0, shard=lax.rem(me + off, n)).start()

    @pl.when(~last_place)
    def _():
        send_early(UP).start()

    @pl.when(~first_place)
    def _():
        send_early(DOWN).start()

    send_early(ACROSS).start()
    mix_and_sum(1)
    sum_copy(n + m, n + m + 1, 2, **targets[ACROSS]).start()
    scale = own(0)
    took(gains, small_sem.at[1])
    few = gains.shape[2]
    per = lanes // few
    lane = lax.broadcasted_iota(jnp.int32, (1, lanes), 1)
    summed = jnp.concatenate([gains[0] + gains[1]] * per, axis=1)
    norm[mine] = jnp.where(lane // few == mine % per, summed, 0.0)

    @pl.loop(1, parts)
    def _(off):
        norm_row(off).start()

    @pl.when(~first_place)
    def _():
        take_early(UP, place - 1, side, scale)

    @pl.when(~last_place)
    def _():
        take_early(DOWN, place + 1, side, scale)

    take_early(ACROSS, place, 1 - side, scale)
    own(1)
    took(norm.at[pl.ds(0, parts - 1)], norm_sem.at[1])

    @pl.loop(1, n)
    def _(off):
        norm_group(off).start()

    def set_aside(i, j, c):
        @pl.loop(0, tall // 8)
        def _(r):
            at = (c // half * n + 2 * j + side) * rows + c % half * tall + r * 8
            left[pl.ds(pl.multiple_of(i * tall + r * 8, 8), 8)] = held[pl.ds(pl.multiple_of(at, 8), 8)]

    @pl.when((place == 1) | (place == m - 2))
    def _():
        for i in range(max(along for along, _ in lates)):
            set_aside(i, place, pieces - 1 - 2 * i)

    line.relay()

    @pl.when(first_place | last_place)
    def _():
        for i in range(max(across for _, across in lates)):
            set_aside(i, jnp.where(first_place, m - 1, 0), pieces - 1 - i)

    took(norm.at[pl.ds(0, (n - 1) * parts)], norm_sem.at[2])

    @pl.loop(0, gain.shape[0])
    def _(r):
        gain_rows[pl.ds(r, 1)] = functools.reduce(lambda t, i: t + norm[r * per + i], range(1, per), norm[r * per])

    gain[...] = gain_rows[...].astype(jnp.bfloat16)

    line.finish()
    took(sums.at[pl.ds(0, n - 1 + m)], sum_send.at[0])
    took(norm.at[pl.ds(0, n * parts - 1)], norm_sem.at[0])

    @pl.when(first_place | last_place)
    def _():
        took(early.at[pl.ds(0, 2)], early_send.at[0])

    @pl.when(~(first_place | last_place))
    def _():
        took(early, early_send.at[0])


def last_kernel(n, lates, left, token, more, send_sem, recv_sem):
    tall = left.shape[0] // max(map(max, lates))
    me, turn = lax.axis_index("shard"), lax.axis_index("tp") % 2
    place, side, last = me // 2, me % 2, n // 2 - 1
    ends, nexts = (place == 0) | (place == last), (place == 1) | (place == last - 1)
    partner = {"shard": 2 * place + 1 - side}
    inward = {"shard": jnp.where(place == 0, 2, 2 * last - 2) + side}
    outward = {"shard": jnp.where(place == 1, 0, 2 * last) + side}
    barrier = pltpu.get_barrier_semaphore()

    @pl.when(ends)
    def _():
        for device in (partner, inward):
            pl.semaphore_signal(barrier, inc=1, device_id=device, device_id_type=MESH)
        pl.semaphore_wait(barrier, 2)

    @pl.when(nexts)
    def _():
        pl.semaphore_signal(barrier, inc=1, device_id=outward, device_id_type=MESH)
        pl.semaphore_wait(barrier, 1)

    for t, late in enumerate(lates):
        def copy(which, device, late=late):
            return pltpu.make_async_remote_copy(
                src_ref=left.at[pl.ds(0, late[which] * tall)], dst_ref=more.at[which, pl.ds(0, late[which] * tall)],
                send_sem=send_sem.at[0], recv_sem=recv_sem.at[which],
                device_id=device, device_id_type=MESH,
            )

        @pl.when((turn == t) & nexts)
        def _(copy=copy):
            along = copy(0, outward)
            along.start()
            along.wait_send()

        @pl.when((turn == t) & ends)
        def _(copy=copy):
            across = copy(1, partner)
            across.start()
            copy(0, inward).wait_recv()
            across.wait()


def write_kernel(
    held, factor_gate, factor_up, gain, gate, up, out_gate, out_up, out_gain, token, sem, small_sem,
):
    size = gate.shape[0]
    tall = 64
    token[...] = jnp.zeros_like(token)
    small = [
        pltpu.make_async_copy(source, out, small_sem.at[i])
        for i, (source, out) in enumerate(((factor_gate, out_gate), (factor_up, out_up), (gain, out_gain)))
    ]

    @pl.loop(0, size // tall)
    def _(i):
        at = pl.multiple_of(i * tall, tall)
        for a, out in enumerate((gate, up)):
            pltpu.make_async_copy(held.at[pl.ds(a * size + at, tall)], out.at[pl.ds(at, tall)], sem.at[0]).start()

    for copy in small:
        copy.start()
    for copy in small:
        copy.wait()
    took(held, sem.at[0])


def write_last_kernel(n, pieces, lates, more, gate_in, up_in, gate, up, sem):
    half = pieces // 2
    rows = gate.shape[0] // n
    tall = rows // half
    me = lax.axis_index("shard")
    place, side, last = me // 2, me % 2, n // 2 - 1
    near, far = jnp.where(place == 0, 1, last - 1), jnp.where(place == 0, last, 0)

    for turn, late in enumerate(lates):
        @pl.when((lax.axis_index("tp") % 2 == turn) & ((place == 0) | (place == last)))
        def _(late=late):
            for which, (j, s, step) in enumerate(((near, side, 2), (far, 1 - side, 1))):
                for i in range(late[which]):
                    c = pieces - 1 - step * i
                    at = pl.multiple_of((2 * j + s) * rows + c % half * tall, 8)
                    pltpu.make_async_copy(
                        more.at[which, pl.ds(i * tall, tall)], (gate, up)[c // half].at[pl.ds(at, tall)], sem.at[0]
                    ).start()
            took(gate.at[pl.ds(0, sum(late) * tall)], sem.at[0])


def shards(n, parts, one_gate, other_gate, one_up, other_up, mix_share, norm_train, norm_step):
    rows, cols = one_gate.shape
    few = norm_train.shape[0]
    lanes = 128
    padded = -(-rows // lanes) * lanes
    pieces = 2 * max(1, rows // 32)
    lates = late_of(pieces)
    aside = max(map(max, lates)) * rows // (pieces // 2)
    ahead = max(8, rows // 16 // 8 * 8)
    gain_shape = (n * parts * few // lanes, lanes)
    kinds = pltpu.SemaphoreType
    vmem, anywhere = pl.BlockSpec(memory_space=pltpu.VMEM), pl.BlockSpec(memory_space=pl.ANY)
    blocks = pltpu.VMEM((2 * n * rows, cols), jnp.bfloat16)
    held, left, factor_gate, factor_up, gain = pl.pallas_call(
        functools.partial(gather_kernel, n, parts, pieces, ahead, lates),
        out_shape=(
            blocks,
            pltpu.VMEM((aside, cols), jnp.bfloat16),
            pltpu.VMEM((1, cols), jnp.float32),
            pltpu.VMEM((1, cols), jnp.float32),
            pltpu.VMEM(gain_shape, jnp.bfloat16),
        ),
        in_specs=[pl.BlockSpec(memory_space=pltpu.HBM)] * 7,
        out_specs=(vmem,) * 5,
        scratch_shapes=[
            pltpu.VMEM((2, rows, cols), jnp.float32),
            pltpu.VMEM((2, rows, cols), jnp.float32),
            pltpu.VMEM((n + n // 2 + 2, 1, cols), jnp.float32),
            pltpu.VMEM((1, padded), jnp.float32),
            pltpu.VMEM((padded, lanes), jnp.float32),
            pltpu.VMEM((2, 1, few), jnp.float32),
            pltpu.VMEM((n * parts, 1, lanes), jnp.float32),
            pltpu.VMEM(gain_shape, jnp.float32),
            pltpu.VMEM((3, ahead, cols), jnp.float32),
            kinds.DMA((1,)),
            kinds.DMA((3,)),
            kinds.DMA((pieces,)),
            kinds.DMA((2,)),
            kinds.DMA((1,)),
            kinds.DMA((3,)),
            kinds.DMA((3,)),
            kinds.DMA((3,)),
            kinds.DMA((n // 2, pieces)),
            kinds.DMA((1,)),
        ],
        compiler_params=pltpu.CompilerParams(
            collective_id=0, has_side_effects=True, vmem_limit_bytes=46 * 2**20
        ),
        name="mix_gather",
    )(
        one_gate, other_gate, one_up, other_up,
        jnp.pad(mix_share, (0, padded - rows))[None], norm_train[None], norm_step[None],
    )
    small = pltpu.CompilerParams(vmem_limit_bytes=2**20)
    whole = (jax.ShapeDtypeStruct((n * rows, cols), jnp.bfloat16),) * 2
    gate, up, factor_gate, factor_up, gain, token = pl.pallas_call(
        write_kernel,
        out_shape=whole + (jax.ShapeDtypeStruct((1, cols), jnp.float32),) * 2
        + (jax.ShapeDtypeStruct(gain_shape, jnp.bfloat16), pltpu.VMEM((8, lanes), jnp.float32)),
        in_specs=[vmem] * 4,
        out_specs=(anywhere,) * 5 + (vmem,),
        scratch_shapes=[kinds.DMA((1,)), kinds.DMA((3,))],
        compiler_params=small,
        name="write_out",
    )(held, factor_gate, factor_up, gain)
    more = pl.pallas_call(
        functools.partial(last_kernel, n, lates),
        out_shape=pltpu.VMEM((2, aside, cols), jnp.bfloat16),
        in_specs=[vmem] * 2,
        out_specs=vmem,
        scratch_shapes=[kinds.DMA((1,)), kinds.DMA((2,))],
        compiler_params=pltpu.CompilerParams(collective_id=1, has_side_effects=True, vmem_limit_bytes=2**20),
        name="gather_last",
    )(left, token)
    gate, up = pl.pallas_call(
        functools.partial(write_last_kernel, n, pieces, lates),
        out_shape=whole,
        in_specs=[vmem, anywhere, anywhere],
        out_specs=(anywhere,) * 2,
        input_output_aliases={1: 0, 2: 1},
        scratch_shapes=[kinds.DMA((1,))],
        compiler_params=small,
        name="write_last",
    )(more, gate, up)
    return gate, up, factor_gate[0], factor_up[0], gain.reshape(-1)


def solution(mesh):
    return jax.shard_map(
        functools.partial(shards, mesh.shape["shard"], mesh.shape["tp"]),
        mesh=mesh,
        in_specs=(
            P("shard", "tp"),
            P("shard", "tp"),
            P("shard", "tp"),
            P("shard", "tp"),
            P("shard"),
            P(("shard", "tp")),
            P(("shard", "tp")),
        ),
        out_specs=(P(None, "tp"), P(None, "tp"), P("tp"), P("tp"), P()),
        check_vma=False,
    )
```

```python
import functools

import jax
import jax.numpy as jnp
import numpy as np
from jax import lax
from jax.experimental import pallas as pl
from jax.experimental.pallas import tpu as pltpu
from jax.sharding import PartitionSpec as P

MESH = pl.DeviceIdType.MESH
UP, DOWN, ACROSS = 0, 1, 2
LATE = ((1, 1), (10, 10))


def crosses(place, m, j, c):
    last = m - 1
    kept = ((place == 0) & (j == 1)) | ((place == last) & (j == last - 1))
    kept = kept & (c % 2 == 1)
    return ~(kept | ((place == 1) & (j == 0)) | ((place == last - 1) & (j == last)))


def sent(m, pieces, late, place):
    last, count = m - 1, pieces
    extra = count if place in (0, last) else 0
    inner = pieces // 2 if place in (1, last - 1) else 0
    up = (place + 1) * count * (place != last) + extra * (place == 0) + inner * (place == last - 1)
    down = (m - place) * count * (place != 0) + extra * (place == last) + inner * (place == 1)
    across = count + sum(
        bool(crosses(np.int64(place), m, np.int64(j), np.int64(c)))
        for j in range(m) if j != place for c in range(pieces)
    )
    return up - late[0] * (place == last - 1), down - late[0] * (place == 1), across - late[1] * (place in (0, last))


def late_of(pieces):
    return tuple((min(along, pieces // 2 + pieces // 4), min(across, pieces - 1)) for along, across in LATE)


def took(ref, sem):
    pltpu.make_async_copy(ref, ref, sem).wait()


class Line:
    def __init__(self, n, pieces, rows, lates, land, send_sem, recv_sem, rest_sem, ahead):
        self.n, self.m, self.half = n, n // 2, pieces // 2
        self.rows, self.tall, self.pieces, self.lates, self.ahead = rows, rows // (pieces // 2), pieces, lates, ahead
        self.me = lax.axis_index("shard")
        self.place, self.side = self.me // 2, self.me % 2
        self.turn = lax.axis_index("tp") % 2
        self.along, self.across = (jnp.where(self.turn == 0, *counts) for counts in zip(*lates))
        self.land = land
        self.send_sem, self.recv_sem, self.rest_sem = send_sem, recv_sem, rest_sem
        self.first, self.last = self.place == 0, self.place == self.m - 1
        me = self.me
        self.targets = {
            UP: {"shard": lax.rem(me + 2, n)},
            DOWN: {"shard": lax.rem(me + n - 2, n)},
            ACROSS: {"shard": 2 * self.place + 1 - self.side},
        }

    def late_along(self, c):
        return (c % 2 == 1) & (c >= self.pieces - 2 * self.along)

    def late_passed(self, c):
        return (c % 2 == 1) & (c >= 2 * self.pieces - 2 * self.along)

    def late_across(self, j, c):
        far = jnp.where(self.first, self.m - 1, 0)
        return (self.first | self.last) & (j == far) & (c >= self.pieces - self.across)

    def piece(self, ref, j, s, c, skip=0):
        at = (c // self.half * self.n + 2 * j + s) * self.rows + c % self.half * self.tall + skip
        return ref.at[pl.ds(pl.multiple_of(at, 8), self.tall - skip)]

    def send(self, way, j, s, c, rest=False, skip=0):
        block = self.piece(self.land, j, s, c, skip)
        return pltpu.make_async_remote_copy(
            src_ref=block, dst_ref=block,
            send_sem=self.send_sem.at[way], recv_sem=self.rest_sem.at[0] if rest else self.recv_sem.at[j, c],
            device_id=self.targets[way], device_id_type=MESH,
        )

    def send_own(self, c, skip=0):
        late = self.late_along(c)

        @pl.when(~(self.last | ((self.place == self.m - 2) & late)))
        def _():
            self.send(UP, self.place, self.side, c, False, skip).start()

        @pl.when(~(self.first | ((self.place == 1) & late)))
        def _():
            self.send(DOWN, self.place, self.side, c, False, skip).start()

        self.send(ACROSS, self.place, self.side, c, False, skip).start()

    def arrived(self, j, s, c, first):
        def whole():
            took(self.piece(self.land, j, s, c), self.recv_sem.at[j, c])

        if not self.ahead:
            return whole()

        @pl.when(first)
        def _():
            took(self.piece(self.land, j, s, c, self.ahead), self.recv_sem.at[j, c])

        pl.when(~first)(whole)

    def relay(self):
        place, side, m, last = self.place, self.side, self.m, self.m - 1
        ends, inner = self.first | self.last, (place == 1) | (place == last - 1)

        @pl.loop(0, last)
        def _(b):
            @pl.loop(0, self.pieces)
            def _(c):
                late = self.late_along(c) & (b == 0)

                def pass_on(way, j, stop):
                    self.arrived(j, side, c, (b == 0) & (c == 0))

                    @pl.when(~stop)
                    def _():
                        self.send(way, j, side, c).start()

                    @pl.when(crosses(place, m, j, c) & ~self.late_across(j, c))
                    def _():
                        self.send(ACROSS, j, side, c, True).start()

                @pl.when((b < place) & ~(self.last & late))
                def _():
                    pass_on(UP, place - 1 - b, self.last)

                @pl.when((b < last - place) & ~(self.first & late))
                def _():
                    pass_on(DOWN, place + 1 + b, self.first)

                @pl.when((ends & (b == 1)) | (inner & (b == last - 1) & (c % 2 == 1)))
                def _():
                    self.arrived(place, 1 - side, c, c == 0)
                    now = ~(inner & self.late_passed(c))

                    @pl.when((self.first | (place == last - 1)) & now)
                    def _():
                        self.send(UP, place, 1 - side, c, True).start()

                    @pl.when((self.last | (place == 1)) & now)
                    def _():
                        self.send(DOWN, place, 1 - side, c, True).start()

    def finish(self):
        place, side, last = self.place, self.side, self.m - 1
        ends, inner = self.first | self.last, (place == 1) | (place == last - 1)

        @pl.loop(0, self.pieces)
        def _(c):
            @pl.when(~(ends | (inner & (c % 2 == 1))))
            def _():
                self.arrived(place, 1 - side, c, c == 0)

        for turn, late in enumerate(self.lates):
            for k in range(self.m):
                @pl.when((self.turn == turn) & (place == k))
                def _(late=late, k=k):
                    passed = max(0, late[0] - self.pieces // 2)
                    rest = last * self.pieces - (late[1] + passed) * (k in (0, last))
                    took(self.land.at[pl.ds(0, rest * self.tall)], self.rest_sem.at[0])
                    for way, count in enumerate(sent(self.m, self.pieces, late, k)):
                        if count:
                            took(self.land.at[pl.ds(0, count * self.tall - self.ahead)], self.send_sem.at[way])


def gather_kernel(
    n, parts, pieces, ahead, lates, one_gate, other_gate, one_up, other_up, mix, train, step,
    held, left, factor_gate, factor_up, gain,
    ones, others, sums, mix_row, shares, gains, norm, gain_rows, early,
    early_send, early_recv, in_sem, small_sem, sum_send, sum_recv, norm_sem, send_sem, recv_sem, rest_sem,
):
    me = lax.axis_index("shard")
    part = lax.axis_index("tp")
    m, half = n // 2, pieces // 2
    place, side = me // 2, me % 2
    rows, cols = ones.shape[1:]
    tall = rows // half
    mine = me * parts + part
    line = Line(n, pieces, rows, lates, held, send_sem, recv_sem, rest_sem, ahead)
    targets, first_place, last_place = line.targets, line.first, line.last
    lanes = shares.shape[1]

    read_mix = pltpu.make_async_copy(mix, mix_row, small_sem.at[0])
    read_mix.start()
    barrier = pltpu.get_barrier_semaphore()

    @pl.loop(1, n)
    def _(off):
        pl.semaphore_signal(barrier, inc=1, device_id={"shard": lax.rem(me + off, n)}, device_id_type=MESH)

    @pl.loop(1, parts)
    def _(off):
        pl.semaphore_signal(barrier, inc=1, device_id={"tp": lax.rem(part + off, parts)}, device_id_type=MESH)

    read_gains = [
        pltpu.make_async_copy(source, gains.at[i], small_sem.at[1]) for i, source in enumerate((train, step))
    ]

    def reads(piece):
        a, at = piece // half, pl.ds(piece % half * tall, tall)
        first, second = ((one_gate, other_gate), (one_up, other_up))[a]
        return (
            pltpu.make_async_copy(first.at[at], ones.at[a, at], in_sem.at[piece]),
            pltpu.make_async_copy(second.at[at], others.at[a, at], in_sem.at[piece]),
        )

    for piece in range(half):
        for copy in reads(piece):
            copy.start()
    read_mix.wait()
    shares[...] = jnp.transpose(jnp.broadcast_to(mix_row[...], (lanes, shares.shape[0])))

    def mix_and_sum(a):
        total = jnp.zeros((8, cols), jnp.float32)
        for piece in range(a * half, (a + 1) * half):
            took(ones.at[:, pl.ds(0, tall)], in_sem.at[piece])
            if piece == half - 1:
                for later in range(half, pieces):
                    for copy in reads(later):
                        copy.start()
                for copy in read_gains:
                    copy.start()

            def mixed(r, total):
                at = pl.ds(pl.multiple_of(piece % half * tall + r * 8, 8), 8)
                share = shares[at]
                rest = 1.0 - share
                share, rest = (jnp.concatenate([v] * (cols // lanes), axis=1) for v in (share, rest))
                fresh = share * ones[a, at] + rest * others[a, at]
                ones[a, at] = fresh
                return total + fresh * fresh

            total = lax.fori_loop(0, tall // 8, mixed, total, unroll=4)
        sums[(me, n + m)[a]] = jnp.sum(total, axis=0, keepdims=True)

    def sum_copy(source, target, recv, **device_id):
        return pltpu.make_async_remote_copy(
            src_ref=sums.at[source], dst_ref=sums.at[target],
            send_sem=sum_send.at[0], recv_sem=sum_recv.at[recv],
            device_id=device_id, device_id_type=MESH,
        )

    def exchange_up():
        took(sums.at[0], sum_recv.at[2])
        sums[n + place] = sums[n + m] + sums[n + m + 1]

        @pl.loop(1, m)
        def _(off):
            sum_copy(n + place, n + place, 1, shard=lax.rem(me + 2 * off, n)).start()

    def scales(a):
        first, count = ((0, n), (n, m))[a]
        took(sums.at[pl.ds(0, count - 1)], sum_recv.at[a])
        factors = jnp.sqrt(lax.fori_loop(1, count, lambda i, t: t + sums[first + i], sums[first]))
        (factor_gate, factor_up)[a][...] = factors
        return jnp.broadcast_to(1.0 / factors, (8, cols))

    def norm_row(off):
        return pltpu.make_async_remote_copy(
            src_ref=norm.at[mine], dst_ref=norm.at[mine],
            send_sem=norm_sem.at[0], recv_sem=norm_sem.at[1],
            device_id={"tp": lax.rem(part + off, parts)}, device_id_type=MESH,
        )

    def norm_group(off):
        return pltpu.make_async_remote_copy(
            src_ref=norm.at[pl.ds(me * parts, parts)], dst_ref=norm.at[pl.ds(me * parts, parts)],
            send_sem=norm_sem.at[0], recv_sem=norm_sem.at[2],
            device_id={"shard": lax.rem(me + off, n)}, device_id_type=MESH,
        )

    def send_early(way):
        return pltpu.make_async_remote_copy(
            src_ref=ones.at[0, pl.ds(0, ahead)], dst_ref=early.at[way],
            send_sem=early_send.at[0], recv_sem=early_recv.at[way],
            device_id=targets[way], device_id_type=MESH,
        )

    def take_early(way, j, s, scale):
        took(early.at[way], early_recv.at[way])
        for r in range(0, ahead, 8):
            there = pl.multiple_of((2 * j + s) * rows + r, 8)
            held[pl.ds(there, 8)] = (early[way, pl.ds(r, 8)] * scale).astype(jnp.bfloat16)

    def own(a):
        scale = scales(a)
        for c in range(a * half, (a + 1) * half):
            at = c % half * tall
            skip = ahead if c == 0 else 0

            def scaled(r, _):
                here = pl.multiple_of(at + r * 8, 8)
                there = pl.multiple_of((a * n + me) * rows + at + r * 8, 8)
                held[pl.ds(there, 8)] = (ones[a, pl.ds(here, 8)] * scale).astype(jnp.bfloat16)
                return 0

            lax.fori_loop(0, tall // 8, scaled, 0, unroll=4)
            line.send_own(c, skip)
            if c == (half - 1) // 2:
                exchange_up()
        return scale

    mix_and_sum(0)
    pl.semaphore_wait(barrier, n + parts - 2)

    @pl.loop(1, n)
    def _(off):
        sum_copy(me, me, 0, shard=lax.rem(me + off, n)).start()

    @pl.when(~last_place)
    def _():
        send_early(UP).start()

    @pl.when(~first_place)
    def _():
        send_early(DOWN).start()

    send_early(ACROSS).start()
    mix_and_sum(1)
    sum_copy(n + m, n + m + 1, 2, **targets[ACROSS]).start()
    scale = own(0)
    took(gains, small_sem.at[1])
    few = gains.shape[2]
    per = lanes // few
    lane = lax.broadcasted_iota(jnp.int32, (1, lanes), 1)
    summed = jnp.concatenate([gains[0] + gains[1]] * per, axis=1)
    norm[mine] = jnp.where(lane // few == mine % per, summed, 0.0)

    @pl.loop(1, parts)
    def _(off):
        norm_row(off).start()

    @pl.when(~first_place)
    def _():
        take_early(UP, place - 1, side, scale)

    @pl.when(~last_place)
    def _():
        take_early(DOWN, place + 1, side, scale)

    take_early(ACROSS, place, 1 - side, scale)
    own(1)
    took(norm.at[pl.ds(0, parts - 1)], norm_sem.at[1])

    @pl.loop(1, n)
    def _(off):
        norm_group(off).start()

    def set_aside(i, j, c, side=side):
        @pl.loop(0, tall // 8)
        def _(r):
            at = (c // half * n + 2 * j + side) * rows + c % half * tall + r * 8
            left[pl.ds(pl.multiple_of(i * tall + r * 8, 8), 8)] = held[pl.ds(pl.multiple_of(at, 8), 8)]

    line.relay()

    @pl.when((place == 1) | (place == m - 2))
    def _():
        for i in range(max(along for along, _ in lates)):
            set_aside(i, place, pieces - 1 - 2 * (i % half), (side, 1 - side)[i // half])

    @pl.when(first_place | last_place)
    def _():
        for i in range(max(across for _, across in lates)):
            set_aside(i, jnp.where(first_place, m - 1, 0), pieces - 1 - i)

    took(norm.at[pl.ds(0, (n - 1) * parts)], norm_sem.at[2])

    @pl.loop(0, gain.shape[0])
    def _(r):
        gain_rows[pl.ds(r, 1)] = functools.reduce(lambda t, i: t + norm[r * per + i], range(1, per), norm[r * per])

    gain[...] = gain_rows[...].astype(jnp.bfloat16)

    line.finish()
    took(sums.at[pl.ds(0, n - 1 + m)], sum_send.at[0])
    took(norm.at[pl.ds(0, n * parts - 1)], norm_sem.at[0])

    @pl.when(first_place | last_place)
    def _():
        took(early.at[pl.ds(0, 2)], early_send.at[0])

    @pl.when(~(first_place | last_place))
    def _():
        took(early, early_send.at[0])


def last_kernel(n, lates, left, token, more, send_sem, recv_sem):
    tall = left.shape[0] // max(map(max, lates))
    me, turn = lax.axis_index("shard"), lax.axis_index("tp") % 2
    place, side, last = me // 2, me % 2, n // 2 - 1
    ends, nexts = (place == 0) | (place == last), (place == 1) | (place == last - 1)
    partner = {"shard": 2 * place + 1 - side}
    inward = {"shard": jnp.where(place == 0, 2, 2 * last - 2) + side}
    outward = {"shard": jnp.where(place == 1, 0, 2 * last) + side}
    barrier = pltpu.get_barrier_semaphore()

    @pl.when(ends)
    def _():
        for device in (partner, inward):
            pl.semaphore_signal(barrier, inc=1, device_id=device, device_id_type=MESH)
        pl.semaphore_wait(barrier, 2)

    @pl.when(nexts)
    def _():
        pl.semaphore_signal(barrier, inc=1, device_id=outward, device_id_type=MESH)
        pl.semaphore_wait(barrier, 1)

    for t, late in enumerate(lates):
        def copy(which, device, late=late):
            return pltpu.make_async_remote_copy(
                src_ref=left.at[pl.ds(0, late[which] * tall)], dst_ref=more.at[which, pl.ds(0, late[which] * tall)],
                send_sem=send_sem.at[0], recv_sem=recv_sem.at[which],
                device_id=device, device_id_type=MESH,
            )

        @pl.when((turn == t) & nexts)
        def _(copy=copy):
            along = copy(0, outward)
            along.start()
            along.wait_send()

        @pl.when((turn == t) & ends)
        def _(copy=copy):
            across = copy(1, partner)
            across.start()
            copy(0, inward).wait_recv()
            across.wait()


def write_kernel(
    held, factor_gate, factor_up, gain, gate, up, out_gate, out_up, out_gain, token, sem, small_sem,
):
    size = gate.shape[0]
    tall = 64
    token[...] = jnp.zeros_like(token)
    small = [
        pltpu.make_async_copy(source, out, small_sem.at[i])
        for i, (source, out) in enumerate(((factor_gate, out_gate), (factor_up, out_up), (gain, out_gain)))
    ]

    @pl.loop(0, size // tall)
    def _(i):
        at = pl.multiple_of(i * tall, tall)
        for a, out in enumerate((gate, up)):
            pltpu.make_async_copy(held.at[pl.ds(a * size + at, tall)], out.at[pl.ds(at, tall)], sem.at[0]).start()

    for copy in small:
        copy.start()
    for copy in small:
        copy.wait()
    took(held, sem.at[0])


def write_last_kernel(n, pieces, lates, more, gate_in, up_in, gate, up, sem):
    half = pieces // 2
    rows = gate.shape[0] // n
    tall = rows // half
    me = lax.axis_index("shard")
    place, side, last = me // 2, me % 2, n // 2 - 1
    near, far = jnp.where(place == 0, 1, last - 1), jnp.where(place == 0, last, 0)

    for turn, late in enumerate(lates):
        @pl.when((lax.axis_index("tp") % 2 == turn) & ((place == 0) | (place == last)))
        def _(late=late):
            for which, (j, s, step) in enumerate(((near, side, 2), (far, 1 - side, 1))):
                for i in range(late[which]):
                    c = pieces - 1 - step * (i % half if step == 2 else i)
                    here = 1 - s if step == 2 and i >= half else s
                    at = pl.multiple_of((2 * j + here) * rows + c % half * tall, 8)
                    pltpu.make_async_copy(
                        more.at[which, pl.ds(i * tall, tall)], (gate, up)[c // half].at[pl.ds(at, tall)], sem.at[0]
                    ).start()
            took(gate.at[pl.ds(0, sum(late) * tall)], sem.at[0])


def shards(n, parts, one_gate, other_gate, one_up, other_up, mix_share, norm_train, norm_step):
    rows, cols = one_gate.shape
    few = norm_train.shape[0]
    lanes = 128
    padded = -(-rows // lanes) * lanes
    pieces = 2 * max(1, rows // 32)
    lates = late_of(pieces)
    aside = max(map(max, lates)) * rows // (pieces // 2)
    ahead = max(8, rows // 16 // 8 * 8)
    gain_shape = (n * parts * few // lanes, lanes)
    kinds = pltpu.SemaphoreType
    vmem, anywhere = pl.BlockSpec(memory_space=pltpu.VMEM), pl.BlockSpec(memory_space=pl.ANY)
    blocks = pltpu.VMEM((2 * n * rows, cols), jnp.bfloat16)
    held, left, factor_gate, factor_up, gain = pl.pallas_call(
        functools.partial(gather_kernel, n, parts, pieces, ahead, lates),
        out_shape=(
            blocks,
            pltpu.VMEM((aside, cols), jnp.bfloat16),
            pltpu.VMEM((1, cols), jnp.float32),
            pltpu.VMEM((1, cols), jnp.float32),
            pltpu.VMEM(gain_shape, jnp.bfloat16),
        ),
        in_specs=[pl.BlockSpec(memory_space=pltpu.HBM)] * 7,
        out_specs=(vmem,) * 5,
        scratch_shapes=[
            pltpu.VMEM((2, rows, cols), jnp.float32),
            pltpu.VMEM((2, rows, cols), jnp.float32),
            pltpu.VMEM((n + n // 2 + 2, 1, cols), jnp.float32),
            pltpu.VMEM((1, padded), jnp.float32),
            pltpu.VMEM((padded, lanes), jnp.float32),
            pltpu.VMEM((2, 1, few), jnp.float32),
            pltpu.VMEM((n * parts, 1, lanes), jnp.float32),
            pltpu.VMEM(gain_shape, jnp.float32),
            pltpu.VMEM((3, ahead, cols), jnp.float32),
            kinds.DMA((1,)),
            kinds.DMA((3,)),
            kinds.DMA((pieces,)),
            kinds.DMA((2,)),
            kinds.DMA((1,)),
            kinds.DMA((3,)),
            kinds.DMA((3,)),
            kinds.DMA((3,)),
            kinds.DMA((n // 2, pieces)),
            kinds.DMA((1,)),
        ],
        compiler_params=pltpu.CompilerParams(
            collective_id=0, has_side_effects=True, vmem_limit_bytes=46 * 2**20
        ),
        name="mix_gather",
    )(
        one_gate, other_gate, one_up, other_up,
        jnp.pad(mix_share, (0, padded - rows))[None], norm_train[None], norm_step[None],
    )
    small = pltpu.CompilerParams(vmem_limit_bytes=2**20)
    whole = (jax.ShapeDtypeStruct((n * rows, cols), jnp.bfloat16),) * 2
    gate, up, factor_gate, factor_up, gain, token = pl.pallas_call(
        write_kernel,
        out_shape=whole + (jax.ShapeDtypeStruct((1, cols), jnp.float32),) * 2
        + (jax.ShapeDtypeStruct(gain_shape, jnp.bfloat16), pltpu.VMEM((8, lanes), jnp.float32)),
        in_specs=[vmem] * 4,
        out_specs=(anywhere,) * 5 + (vmem,),
        scratch_shapes=[kinds.DMA((1,)), kinds.DMA((3,))],
        compiler_params=small,
        name="write_out",
    )(held, factor_gate, factor_up, gain)
    more = pl.pallas_call(
        functools.partial(last_kernel, n, lates),
        out_shape=pltpu.VMEM((2, aside, cols), jnp.bfloat16),
        in_specs=[vmem] * 2,
        out_specs=vmem,
        scratch_shapes=[kinds.DMA((1,)), kinds.DMA((2,))],
        compiler_params=pltpu.CompilerParams(collective_id=1, has_side_effects=True, vmem_limit_bytes=2**20),
        name="gather_last",
    )(left, token)
    gate, up = pl.pallas_call(
        functools.partial(write_last_kernel, n, pieces, lates),
        out_shape=whole,
        in_specs=[vmem, anywhere, anywhere],
        out_specs=(anywhere,) * 2,
        input_output_aliases={1: 0, 2: 1},
        scratch_shapes=[kinds.DMA((1,))],
        compiler_params=small,
        name="write_last",
    )(more, gate, up)
    return gate, up, factor_gate[0], factor_up[0], gain.reshape(-1)


def solution(mesh):
    return jax.shard_map(
        functools.partial(shards, mesh.shape["shard"], mesh.shape["tp"]),
        mesh=mesh,
        in_specs=(
            P("shard", "tp"),
            P("shard", "tp"),
            P("shard", "tp"),
            P("shard", "tp"),
            P("shard"),
            P(("shard", "tp")),
            P(("shard", "tp")),
        ),
        out_specs=(P(None, "tp"), P(None, "tp"), P("tp"), P("tp"), P()),
        check_vma=False,
    )
```

```python
import functools

import jax
import jax.numpy as jnp
import numpy as np
from jax import lax
from jax.experimental import pallas as pl
from jax.experimental.pallas import tpu as pltpu
from jax.sharding import PartitionSpec as P

MESH = pl.DeviceIdType.MESH
UP, DOWN, ACROSS = 0, 1, 2
LATE = ((1, 1), (10, 10))


def crosses(place, m, j, c):
    last = m - 1
    kept = ((place == 0) & (j == 1)) | ((place == last) & (j == last - 1))
    kept = kept & (c % 2 == 1)
    return ~(kept | ((place == 1) & (j == 0)) | ((place == last - 1) & (j == last)))


def sent(m, pieces, late, place):
    last, count = m - 1, pieces
    extra = count if place in (0, last) else 0
    inner = pieces // 2 if place in (1, last - 1) else 0
    up = (place + 1) * count * (place != last) + extra * (place == 0) + inner * (place == last - 1)
    down = (m - place) * count * (place != 0) + extra * (place == last) + inner * (place == 1)
    across = count + sum(
        bool(crosses(np.int64(place), m, np.int64(j), np.int64(c)))
        for j in range(m) if j != place for c in range(pieces)
    )
    return up - late[0] * (place == last - 1), down - late[0] * (place == 1), across - late[1] * (place in (0, last))


def late_of(pieces):
    return tuple((min(along, pieces // 2 + pieces // 4), min(across, pieces - 1)) for along, across in LATE)


def took(ref, sem):
    pltpu.make_async_copy(ref, ref, sem).wait()


class Line:
    def __init__(self, n, pieces, rows, lates, land, send_sem, recv_sem, rest_sem, ahead):
        self.n, self.m, self.half = n, n // 2, pieces // 2
        self.rows, self.tall, self.pieces, self.lates, self.ahead = rows, rows // (pieces // 2), pieces, lates, ahead
        self.me = lax.axis_index("shard")
        self.place, self.side = self.me // 2, self.me % 2
        self.turn = lax.axis_index("tp") % 2
        self.along, self.across = (jnp.where(self.turn == 0, *counts) for counts in zip(*lates))
        self.land = land
        self.send_sem, self.recv_sem, self.rest_sem = send_sem, recv_sem, rest_sem
        self.first, self.last = self.place == 0, self.place == self.m - 1
        me = self.me
        self.targets = {
            UP: {"shard": lax.rem(me + 2, n)},
            DOWN: {"shard": lax.rem(me + n - 2, n)},
            ACROSS: {"shard": 2 * self.place + 1 - self.side},
        }

    def late_along(self, c):
        return (c % 2 == 1) & (c >= self.pieces - 2 * self.along)

    def late_passed(self, c):
        return (c % 2 == 1) & (c >= 2 * self.pieces - 2 * self.along)

    def late_across(self, j, c):
        far = jnp.where(self.first, self.m - 1, 0)
        return (self.first | self.last) & (j == far) & (c >= self.pieces - self.across)

    def piece(self, ref, j, s, c, skip=0):
        at = (c // self.half * self.n + 2 * j + s) * self.rows + c % self.half * self.tall + skip
        return ref.at[pl.ds(pl.multiple_of(at, 8), self.tall - skip)]

    def send(self, way, j, s, c, rest=False, skip=0):
        block = self.piece(self.land, j, s, c, skip)
        return pltpu.make_async_remote_copy(
            src_ref=block, dst_ref=block,
            send_sem=self.send_sem.at[way], recv_sem=self.rest_sem.at[0] if rest else self.recv_sem.at[j, c],
            device_id=self.targets[way], device_id_type=MESH,
        )

    def send_own(self, c, skip=0):
        late = self.late_along(c)

        @pl.when(~(self.last | ((self.place == self.m - 2) & late)))
        def _():
            self.send(UP, self.place, self.side, c, False, skip).start()

        @pl.when(~(self.first | ((self.place == 1) & late)))
        def _():
            self.send(DOWN, self.place, self.side, c, False, skip).start()

        self.send(ACROSS, self.place, self.side, c, False, skip).start()

    def arrived(self, j, s, c, first):
        def whole():
            took(self.piece(self.land, j, s, c), self.recv_sem.at[j, c])

        if not self.ahead:
            return whole()

        @pl.when(first)
        def _():
            took(self.piece(self.land, j, s, c, self.ahead), self.recv_sem.at[j, c])

        pl.when(~first)(whole)

    def relay(self):
        place, side, m, last = self.place, self.side, self.m, self.m - 1
        ends, inner = self.first | self.last, (place == 1) | (place == last - 1)

        @pl.loop(0, last)
        def _(b):
            @pl.loop(0, self.pieces)
            def _(c):
                late = self.late_along(c) & (b == 0)

                def pass_on(way, j, stop):
                    self.arrived(j, side, c, (b == 0) & (c == 0))

                    @pl.when(~stop)
                    def _():
                        self.send(way, j, side, c).start()

                    @pl.when(crosses(place, m, j, c) & ~self.late_across(j, c))
                    def _():
                        self.send(ACROSS, j, side, c, True).start()

                @pl.when((b < place) & ~(self.last & late))
                def _():
                    pass_on(UP, place - 1 - b, self.last)

                @pl.when((b < last - place) & ~(self.first & late))
                def _():
                    pass_on(DOWN, place + 1 + b, self.first)

                @pl.when((ends & (b == 1)) | (inner & (b == last - 1) & (c % 2 == 1)))
                def _():
                    self.arrived(place, 1 - side, c, c == 0)
                    now = ~(inner & self.late_passed(c))

                    @pl.when((self.first | (place == last - 1)) & now)
                    def _():
                        self.send(UP, place, 1 - side, c, True).start()

                    @pl.when((self.last | (place == 1)) & now)
                    def _():
                        self.send(DOWN, place, 1 - side, c, True).start()

    def finish(self):
        place, side, last = self.place, self.side, self.m - 1
        ends, inner = self.first | self.last, (place == 1) | (place == last - 1)

        @pl.loop(0, self.pieces)
        def _(c):
            @pl.when(~(ends | (inner & (c % 2 == 1))))
            def _():
                self.arrived(place, 1 - side, c, c == 0)

        for turn, late in enumerate(self.lates):
            for k in range(self.m):
                @pl.when((self.turn == turn) & (place == k))
                def _(late=late, k=k):
                    passed = max(0, late[0] - self.pieces // 2)
                    rest = last * self.pieces - (late[1] + passed) * (k in (0, last))
                    took(self.land.at[pl.ds(0, rest * self.tall)], self.rest_sem.at[0])
                    for way, count in enumerate(sent(self.m, self.pieces, late, k)):
                        if count:
                            took(self.land.at[pl.ds(0, count * self.tall - self.ahead)], self.send_sem.at[way])


def gather_kernel(
    n, parts, pieces, ahead, lates, one_gate, other_gate, one_up, other_up, mix, train, step,
    held, left, factor_gate, factor_up, gain,
    ones, others, sums, mix_row, shares, gains, norm, gain_rows, early,
    early_send, early_recv, in_sem, small_sem, sum_send, sum_recv, norm_sem, send_sem, recv_sem, rest_sem,
):
    me = lax.axis_index("shard")
    part = lax.axis_index("tp")
    m, half = n // 2, pieces // 2
    place, side = me // 2, me % 2
    rows, cols = ones.shape[1:]
    tall = rows // half
    mine = me * parts + part
    group = 2 - half % 2
    line = Line(n, pieces, rows, lates, held, send_sem, recv_sem, rest_sem, ahead)
    targets, first_place, last_place = line.targets, line.first, line.last
    lanes = shares.shape[1]

    read_mix = pltpu.make_async_copy(mix, mix_row, small_sem.at[0])
    read_mix.start()
    barrier = pltpu.get_barrier_semaphore()

    @pl.loop(1, n)
    def _(off):
        pl.semaphore_signal(barrier, inc=1, device_id={"shard": lax.rem(me + off, n)}, device_id_type=MESH)

    @pl.loop(1, parts)
    def _(off):
        pl.semaphore_signal(barrier, inc=1, device_id={"tp": lax.rem(part + off, parts)}, device_id_type=MESH)

    read_gains = [
        pltpu.make_async_copy(source, gains.at[i], small_sem.at[1]) for i, source in enumerate((train, step))
    ]

    def reads(piece):
        a, at = piece // half, pl.ds(piece % half * tall, tall)
        first, second = ((one_gate, other_gate), (one_up, other_up))[a]
        return (
            pltpu.make_async_copy(first.at[at], ones.at[a, at], in_sem.at[piece // group]),
            pltpu.make_async_copy(second.at[at], others.at[a, at], in_sem.at[piece // group]),
        )

    for piece in range(half):
        for copy in reads(piece):
            copy.start()
    read_mix.wait()
    shares[...] = jnp.transpose(jnp.broadcast_to(mix_row[...], (lanes, shares.shape[0])))

    def mix_and_sum(a):
        total = jnp.zeros((8, cols), jnp.float32)
        for piece in range(a * half, (a + 1) * half):
            if piece % group == 0:
                took(ones.at[:, pl.ds(0, group * tall)], in_sem.at[piece // group])
            if piece == half - 1:
                for later in range(half, pieces):
                    for copy in reads(later):
                        copy.start()
                for copy in read_gains:
                    copy.start()

            def mixed(r, total):
                at = pl.ds(pl.multiple_of(piece % half * tall + r * 8, 8), 8)
                share = shares[at]
                rest = 1.0 - share
                share, rest = (jnp.concatenate([v] * (cols // lanes), axis=1) for v in (share, rest))
                fresh = share * ones[a, at] + rest * others[a, at]
                ones[a, at] = fresh
                return total + fresh * fresh

            total = lax.fori_loop(0, tall // 8, mixed, total, unroll=4)
        sums[(me, n + m)[a]] = jnp.sum(total, axis=0, keepdims=True)

    def sum_copy(source, target, recv, **device_id):
        return pltpu.make_async_remote_copy(
            src_ref=sums.at[source], dst_ref=sums.at[target],
            send_sem=sum_send.at[0], recv_sem=sum_recv.at[recv],
            device_id=device_id, device_id_type=MESH,
        )

    def exchange_up():
        took(sums.at[0], sum_recv.at[2])
        sums[n + place] = sums[n + m] + sums[n + m + 1]

        @pl.loop(1, m)
        def _(off):
            sum_copy(n + place, n + place, 1, shard=lax.rem(me + 2 * off, n)).start()

    def scales(a):
        first, count = ((0, n), (n, m))[a]
        took(sums.at[pl.ds(0, count - 1)], sum_recv.at[a])
        factors = jnp.sqrt(lax.fori_loop(1, count, lambda i, t: t + sums[first + i], sums[first]))
        (factor_gate, factor_up)[a][...] = factors
        return jnp.broadcast_to(1.0 / factors, (8, cols))

    def norm_row(off):
        return pltpu.make_async_remote_copy(
            src_ref=norm.at[mine], dst_ref=norm.at[mine],
            send_sem=norm_sem.at[0], recv_sem=norm_sem.at[1],
            device_id={"tp": lax.rem(part + off, parts)}, device_id_type=MESH,
        )

    def norm_group(off):
        return pltpu.make_async_remote_copy(
            src_ref=norm.at[pl.ds(me * parts, parts)], dst_ref=norm.at[pl.ds(me * parts, parts)],
            send_sem=norm_sem.at[0], recv_sem=norm_sem.at[2],
            device_id={"shard": lax.rem(me + off, n)}, device_id_type=MESH,
        )

    def send_early(way):
        return pltpu.make_async_remote_copy(
            src_ref=ones.at[0, pl.ds(0, ahead)], dst_ref=early.at[way],
            send_sem=early_send.at[0], recv_sem=early_recv.at[way],
            device_id=targets[way], device_id_type=MESH,
        )

    def take_early(way, j, s, scale):
        took(early.at[way], early_recv.at[way])
        for r in range(0, ahead, 8):
            there = pl.multiple_of((2 * j + s) * rows + r, 8)
            held[pl.ds(there, 8)] = (early[way, pl.ds(r, 8)] * scale).astype(jnp.bfloat16)

    def own(a):
        scale = scales(a)
        for c in range(a * half, (a + 1) * half):
            at = c % half * tall
            skip = ahead if c == 0 else 0

            def scaled(r, _):
                here = pl.multiple_of(at + r * 8, 8)
                there = pl.multiple_of((a * n + me) * rows + at + r * 8, 8)
                held[pl.ds(there, 8)] = (ones[a, pl.ds(here, 8)] * scale).astype(jnp.bfloat16)
                return 0

            lax.fori_loop(0, tall // 8, scaled, 0, unroll=4)
            line.send_own(c, skip)
            if c == (half - 1) // 2:
                exchange_up()
        return scale

    mix_and_sum(0)
    pl.semaphore_wait(barrier, n + parts - 2)

    @pl.loop(1, n)
    def _(off):
        sum_copy(me, me, 0, shard=lax.rem(me + off, n)).start()

    @pl.when(~last_place)
    def _():
        send_early(UP).start()

    @pl.when(~first_place)
    def _():
        send_early(DOWN).start()

    send_early(ACROSS).start()
    mix_and_sum(1)
    sum_copy(n + m, n + m + 1, 2, **targets[ACROSS]).start()
    scale = own(0)
    took(gains, small_sem.at[1])
    few = gains.shape[2]
    per = lanes // few
    lane = lax.broadcasted_iota(jnp.int32, (1, lanes), 1)
    summed = jnp.concatenate([gains[0] + gains[1]] * per, axis=1)
    norm[mine] = jnp.where(lane // few == mine % per, summed, 0.0)

    @pl.loop(1, parts)
    def _(off):
        norm_row(off).start()

    @pl.when(~first_place)
    def _():
        take_early(UP, place - 1, side, scale)

    @pl.when(~last_place)
    def _():
        take_early(DOWN, place + 1, side, scale)

    take_early(ACROSS, place, 1 - side, scale)
    own(1)
    took(norm.at[pl.ds(0, parts - 1)], norm_sem.at[1])

    @pl.loop(1, n)
    def _(off):
        norm_group(off).start()

    def set_aside(i, j, c, side=side):
        @pl.loop(0, tall // 8)
        def _(r):
            at = (c // half * n + 2 * j + side) * rows + c % half * tall + r * 8
            left[pl.ds(pl.multiple_of(i * tall + r * 8, 8), 8)] = held[pl.ds(pl.multiple_of(at, 8), 8)]

    line.relay()

    @pl.when((place == 1) | (place == m - 2))
    def _():
        for i in range(max(along for along, _ in lates)):
            set_aside(i, place, pieces - 1 - 2 * (i % half), (side, 1 - side)[i // half])

    @pl.when(first_place | last_place)
    def _():
        for i in range(max(across for _, across in lates)):
            set_aside(i, jnp.where(first_place, m - 1, 0), pieces - 1 - i)

    took(norm.at[pl.ds(0, (n - 1) * parts)], norm_sem.at[2])

    @pl.loop(0, gain.shape[0])
    def _(r):
        gain_rows[pl.ds(r, 1)] = functools.reduce(lambda t, i: t + norm[r * per + i], range(1, per), norm[r * per])

    gain[...] = gain_rows[...].astype(jnp.bfloat16)

    line.finish()
    took(sums.at[pl.ds(0, n - 1 + m)], sum_send.at[0])
    took(norm.at[pl.ds(0, n * parts - 1)], norm_sem.at[0])

    @pl.when(first_place | last_place)
    def _():
        took(early.at[pl.ds(0, 2)], early_send.at[0])

    @pl.when(~(first_place | last_place))
    def _():
        took(early, early_send.at[0])


def last_kernel(n, lates, left, token, more, send_sem, recv_sem):
    tall = left.shape[0] // max(map(max, lates))
    me, turn = lax.axis_index("shard"), lax.axis_index("tp") % 2
    place, side, last = me // 2, me % 2, n // 2 - 1
    ends, nexts = (place == 0) | (place == last), (place == 1) | (place == last - 1)
    partner = {"shard": 2 * place + 1 - side}
    inward = {"shard": jnp.where(place == 0, 2, 2 * last - 2) + side}
    outward = {"shard": jnp.where(place == 1, 0, 2 * last) + side}
    barrier = pltpu.get_barrier_semaphore()

    @pl.when(ends)
    def _():
        for device in (partner, inward):
            pl.semaphore_signal(barrier, inc=1, device_id=device, device_id_type=MESH)
        pl.semaphore_wait(barrier, 2)

    @pl.when(nexts)
    def _():
        pl.semaphore_signal(barrier, inc=1, device_id=outward, device_id_type=MESH)
        pl.semaphore_wait(barrier, 1)

    for t, late in enumerate(lates):
        def copy(which, device, late=late):
            return pltpu.make_async_remote_copy(
                src_ref=left.at[pl.ds(0, late[which] * tall)], dst_ref=more.at[which, pl.ds(0, late[which] * tall)],
                send_sem=send_sem.at[0], recv_sem=recv_sem.at[which],
                device_id=device, device_id_type=MESH,
            )

        @pl.when((turn == t) & nexts)
        def _(copy=copy):
            along = copy(0, outward)
            along.start()
            along.wait_send()

        @pl.when((turn == t) & ends)
        def _(copy=copy):
            across = copy(1, partner)
            across.start()
            copy(0, inward).wait_recv()
            across.wait()


def write_kernel(
    held, factor_gate, factor_up, gain, gate, up, out_gate, out_up, out_gain, token, sem, small_sem,
):
    size = gate.shape[0]
    tall = 64
    token[...] = jnp.zeros_like(token)
    small = [
        pltpu.make_async_copy(source, out, small_sem.at[i])
        for i, (source, out) in enumerate(((factor_gate, out_gate), (factor_up, out_up), (gain, out_gain)))
    ]

    @pl.loop(0, size // tall)
    def _(i):
        at = pl.multiple_of(i * tall, tall)
        for a, out in enumerate((gate, up)):
            pltpu.make_async_copy(held.at[pl.ds(a * size + at, tall)], out.at[pl.ds(at, tall)], sem.at[0]).start()

    for copy in small:
        copy.start()
    for copy in small:
        copy.wait()
    took(held, sem.at[0])


def write_last_kernel(n, pieces, lates, more, gate_in, up_in, gate, up, sem):
    half = pieces // 2
    rows = gate.shape[0] // n
    tall = rows // half
    me = lax.axis_index("shard")
    place, side, last = me // 2, me % 2, n // 2 - 1
    near, far = jnp.where(place == 0, 1, last - 1), jnp.where(place == 0, last, 0)

    for turn, late in enumerate(lates):
        @pl.when((lax.axis_index("tp") % 2 == turn) & ((place == 0) | (place == last)))
        def _(late=late):
            for which, (j, s, step) in enumerate(((near, side, 2), (far, 1 - side, 1))):
                for i in range(late[which]):
                    c = pieces - 1 - step * (i % half if step == 2 else i)
                    here = 1 - s if step == 2 and i >= half else s
                    at = pl.multiple_of((2 * j + here) * rows + c % half * tall, 8)
                    pltpu.make_async_copy(
                        more.at[which, pl.ds(i * tall, tall)], (gate, up)[c // half].at[pl.ds(at, tall)], sem.at[0]
                    ).start()
            took(gate.at[pl.ds(0, sum(late) * tall)], sem.at[0])


def shards(n, parts, one_gate, other_gate, one_up, other_up, mix_share, norm_train, norm_step):
    rows, cols = one_gate.shape
    few = norm_train.shape[0]
    lanes = 128
    padded = -(-rows // lanes) * lanes
    pieces = 2 * max(1, rows // 32)
    lates = late_of(pieces)
    aside = max(map(max, lates)) * rows // (pieces // 2)
    ahead = max(8, rows // 16 // 8 * 8)
    gain_shape = (n * parts * few // lanes, lanes)
    kinds = pltpu.SemaphoreType
    vmem, anywhere = pl.BlockSpec(memory_space=pltpu.VMEM), pl.BlockSpec(memory_space=pl.ANY)
    blocks = pltpu.VMEM((2 * n * rows, cols), jnp.bfloat16)
    held, left, factor_gate, factor_up, gain = pl.pallas_call(
        functools.partial(gather_kernel, n, parts, pieces, ahead, lates),
        out_shape=(
            blocks,
            pltpu.VMEM((aside, cols), jnp.bfloat16),
            pltpu.VMEM((1, cols), jnp.float32),
            pltpu.VMEM((1, cols), jnp.float32),
            pltpu.VMEM(gain_shape, jnp.bfloat16),
        ),
        in_specs=[pl.BlockSpec(memory_space=pltpu.HBM)] * 7,
        out_specs=(vmem,) * 5,
        scratch_shapes=[
            pltpu.VMEM((2, rows, cols), jnp.float32),
            pltpu.VMEM((2, rows, cols), jnp.float32),
            pltpu.VMEM((n + n // 2 + 2, 1, cols), jnp.float32),
            pltpu.VMEM((1, padded), jnp.float32),
            pltpu.VMEM((padded, lanes), jnp.float32),
            pltpu.VMEM((2, 1, few), jnp.float32),
            pltpu.VMEM((n * parts, 1, lanes), jnp.float32),
            pltpu.VMEM(gain_shape, jnp.float32),
            pltpu.VMEM((3, ahead, cols), jnp.float32),
            kinds.DMA((1,)),
            kinds.DMA((3,)),
            kinds.DMA((pieces // (2 - pieces // 2 % 2),)),
            kinds.DMA((2,)),
            kinds.DMA((1,)),
            kinds.DMA((3,)),
            kinds.DMA((3,)),
            kinds.DMA((3,)),
            kinds.DMA((n // 2, pieces)),
            kinds.DMA((1,)),
        ],
        compiler_params=pltpu.CompilerParams(
            collective_id=0, has_side_effects=True, vmem_limit_bytes=46 * 2**20
        ),
        name="mix_gather",
    )(
        one_gate, other_gate, one_up, other_up,
        jnp.pad(mix_share, (0, padded - rows))[None], norm_train[None], norm_step[None],
    )
    small = pltpu.CompilerParams(vmem_limit_bytes=2**20)
    whole = (jax.ShapeDtypeStruct((n * rows, cols), jnp.bfloat16),) * 2
    gate, up, factor_gate, factor_up, gain, token = pl.pallas_call(
        write_kernel,
        out_shape=whole + (jax.ShapeDtypeStruct((1, cols), jnp.float32),) * 2
        + (jax.ShapeDtypeStruct(gain_shape, jnp.bfloat16), pltpu.VMEM((8, lanes), jnp.float32)),
        in_specs=[vmem] * 4,
        out_specs=(anywhere,) * 5 + (vmem,),
        scratch_shapes=[kinds.DMA((1,)), kinds.DMA((3,))],
        compiler_params=small,
        name="write_out",
    )(held, factor_gate, factor_up, gain)
    more = pl.pallas_call(
        functools.partial(last_kernel, n, lates),
        out_shape=pltpu.VMEM((2, aside, cols), jnp.bfloat16),
        in_specs=[vmem] * 2,
        out_specs=vmem,
        scratch_shapes=[kinds.DMA((1,)), kinds.DMA((2,))],
        compiler_params=pltpu.CompilerParams(collective_id=1, has_side_effects=True, vmem_limit_bytes=2**20),
        name="gather_last",
    )(left, token)
    gate, up = pl.pallas_call(
        functools.partial(write_last_kernel, n, pieces, lates),
        out_shape=whole,
        in_specs=[vmem, anywhere, anywhere],
        out_specs=(anywhere,) * 2,
        input_output_aliases={1: 0, 2: 1},
        scratch_shapes=[kinds.DMA((1,))],
        compiler_params=small,
        name="write_last",
    )(more, gate, up)
    return gate, up, factor_gate[0], factor_up[0], gain.reshape(-1)


def solution(mesh):
    return jax.shard_map(
        functools.partial(shards, mesh.shape["shard"], mesh.shape["tp"]),
        mesh=mesh,
        in_specs=(
            P("shard", "tp"),
            P("shard", "tp"),
            P("shard", "tp"),
            P("shard", "tp"),
            P("shard"),
            P(("shard", "tp")),
            P(("shard", "tp")),
        ),
        out_specs=(P(None, "tp"), P(None, "tp"), P("tp"), P("tp"), P()),
        check_vma=False,
    )
```
